16 devices in a mesh: stage: 2 (over y, z), data: 8 (over x, core).
Axes of the slice: x: 4, y: 2, z: 1, core: 2. Of those that a mesh axis runs over, the one named last changes fastest.
The devices are a block of a 4x4x8 slice.
Arguments:
- w_master: float32 [16, 1024, 2048], P('stage', 'data'), parts along dimension 0
- momentum: float32 [16, 1024, 2048], P('stage', 'data'), parts along dimension 0
- grads: bfloat16 [16, 8, 1024, 2048], P(('stage', 'data')), parts along dimension 0
Outputs:
- output 1: float32 [16, 1024, 2048], P('stage', 'data'), parts along dimension 0
- output 2: float32 [16, 1024, 2048], P('stage', 'data'), parts along dimension 0
There are 2 independent parts. The reference program is written for one: setup_inputs(seed, part) draws one part's arguments, and reference() takes and returns one part's arrays. A program takes and returns all parts, laid end to end along the dimension named above; each array names one.
All inputs are finite; a program needn't handle non-finite values.
Results may differ from the reference program's by a relative error of at most 0.0103596.
Values are sent between devices in bfloat16 or wider.
A program may use at most 768 MiB of HBM per device.

```python
import math
import jax
import jax.numpy as jnp
from jax import lax

GROUP_SIZE = 8
NUM_MATS = 8
MAT_ROWS = 1024
MAT_COLS = 2048
NS_ITERS = 5

MOMENTUM_COEF = 0.95
LEARN_RATE = 0.05
WEIGHT_DECAY = 0.2
NORM_EPS = 1e-7
COEF_A = 3.4445
COEF_B = -4.7750
COEF_C = 2.0315
RMS_SCALE = 0.2 * math.sqrt(max(MAT_ROWS, MAT_COLS))


def setup_inputs(seed: int = 0, part: int = 0) -> dict:
    base_key = jax.random.fold_in(jax.random.key(seed), part)
    sub_keys = jax.random.split(base_key, 6)
    mat_shape = (NUM_MATS, MAT_ROWS, MAT_COLS)
    w_master = 0.02 * jax.random.normal(sub_keys[0], mat_shape, jnp.float32)
    noise_base = jax.random.normal(sub_keys[1], mat_shape, jnp.float32)
    low_left = jax.random.normal(sub_keys[2], (NUM_MATS, MAT_ROWS, 4), jnp.float32)
    low_right = jax.random.normal(sub_keys[3], (NUM_MATS, 4, MAT_COLS), jnp.float32)
    shared = 0.25 * jnp.einsum('mrk,mkc->mrc', low_left, low_right)
    row_scale = jax.random.uniform(sub_keys[4], (NUM_MATS, MAT_ROWS, 1), jnp.float32, 0.5, 1.5)
    momentum = row_scale * (noise_base + shared)
    grads = (jax.random.normal(sub_keys[5], (GROUP_SIZE,) + mat_shape, jnp.float32) * GROUP_SIZE ** -0.5).astype(jnp.bfloat16)
    return {'w_master': w_master, 'momentum': momentum, 'grads': grads}


def newton_schulz(x_start):
    is_tall = MAT_ROWS > MAT_COLS
    x_cur = x_start.T if is_tall else x_start
    for _ in range(NS_ITERS):
        gram_mat = jnp.dot(x_cur, x_cur.T, preferred_element_type=jnp.float32).astype(jnp.bfloat16)
        gram_sq = jnp.dot(gram_mat, gram_mat, preferred_element_type=jnp.float32)
        poly_mat = (COEF_B * gram_mat.astype(jnp.float32) + COEF_C * gram_sq).astype(jnp.bfloat16)
        poly_x = jnp.dot(poly_mat, x_cur, preferred_element_type=jnp.float32)
        x_cur = (COEF_A * x_cur.astype(jnp.float32) + poly_x).astype(jnp.bfloat16)
    return x_cur.T if is_tall else x_cur


def reference(w_master, momentum, grads):
    grad_sum = jnp.sum(grads.astype(jnp.float32), axis=0)
    mom_new = MOMENTUM_COEF * momentum + grad_sum
    frob_norm = jnp.sqrt(jnp.sum(mom_new * mom_new, axis=(1, 2)))

    def one_matrix(mat_pair):
        mom_one, norm_one = mat_pair
        x_start = (mom_one.astype(jnp.bfloat16).astype(jnp.float32) / (norm_one + NORM_EPS)).astype(jnp.bfloat16)
        return newton_schulz(x_start)

    x_ortho = lax.map(one_matrix, (mom_new, frob_norm))
    w_new = w_master - LEARN_RATE * (x_ortho.astype(jnp.float32) * RMS_SCALE + WEIGHT_DECAY * w_master)
    return w_new, mom_new
```

```python
import functools
import math
import jax
import jax.numpy as jnp
from jax import lax
from jax.experimental import pallas as pl
from jax.experimental.pallas import tpu as pltpu
from jax.sharding import PartitionSpec as P

MOMENTUM_COEF = 0.95
LEARN_RATE = 0.05
WEIGHT_DECAY = 0.2
NORM_EPS = 1e-7
COEF_A = 3.4445
COEF_B = -4.7750
COEF_C = 2.0315
NS_ITERS = 5

CORES = 2
AHEAD = 3
CHUNK = 32
ITERS_PER_STEP = 2
MESH = pl.DeviceIdType.MESH
F32 = jnp.float32
BF16 = jnp.bfloat16


def fused_kernel(group, scale, w_ref, mom_ref, g_ref, w_out, mom_out,
                 mg, fin, fsum, own, mout, momin, xmat, gram, poly, ret, nsend, ninbox,
                 s_mg, s_fin, s_fsum, s_own, s_mout, s_mom, s_x, s_n, s_ret,
                 s_gsend, s_xsend, s_nsend, s_rsend, s_momout, s_wload, s_wout):
    n_mats, rows, cols = w_ref.shape
    half = rows // 2
    chips = group // CORES
    n_rows = rows * group
    me = lax.axis_index("data")
    chip, core = me // CORES, me % CORES
    right, left, far = (chip + 1) % chips, (chip + chips - 1) % chips, (chip + 2) % chips

    def dev(a_chip, a_core):
        return a_chip * CORES + a_core

    def owner_of(m):
        return dev(m % chips, m // chips)

    my_mat = (me % CORES) * chips + chip

    def grad_rows(m, a_chip, a_core, h):
        start = pl.multiple_of(dev(a_chip, a_core) * rows + h * half, half)
        return g_ref.at[0, m, pl.ds(start, half)]

    def remote(src, dst, send, recv, to):
        return pltpu.make_async_remote_copy(src_ref=src, dst_ref=dst, send_sem=send, recv_sem=recv,
                                            device_id={"data": to}, device_id_type=MESH)

    def wait_bytes(ref, sem):
        pltpu.make_async_copy(ref, ref, sem).wait()

    def issue_raw(m):
        send = s_gsend.at[m]
        for kk in range(CORES):
            remote(grad_rows(m, far, kk, 0), mg.at[m, 0, core], send, s_mg.at[m, 0], dev(right, kk)).start()
            remote(grad_rows(m, far, kk, 1), mg.at[m, 1, core], send, s_mg.at[m, 1], dev(left, kk)).start()
        mate = dev(chip, 1 - core)
        remote(grad_rows(m, right, 1 - core, 0), mg.at[m, 0, 2], send, s_mg.at[m, 0], mate).start()
        remote(grad_rows(m, left, 1 - core, 1), mg.at[m, 1, 2], send, s_mg.at[m, 1], mate).start()
        for kk in range(CORES):
            remote(grad_rows(m, right, kk, 1), fin.at[m, 1, core], send, s_fin.at[m], dev(right, kk)).start()
            remote(grad_rows(m, left, kk, 0), fin.at[m, 0, core], send, s_fin.at[m], dev(left, kk)).start()
        for h in range(2):
            remote(grad_rows(m, chip, 1 - core, h), fin.at[m, h, 2], send, s_fin.at[m], mate).start()

    def load_own(m):
        slot = m % 3
        pltpu.make_async_copy(grad_rows(m, right, core, 0), own.at[slot, 0], s_own.at[slot]).start()
        pltpu.make_async_copy(grad_rows(m, left, core, 1), own.at[slot, 1], s_own.at[slot]).start()
        for h in range(2):
            pltpu.make_async_copy(grad_rows(m, chip, core, h), own.at[slot, 2 + h], s_own.at[slot]).start()

    def merge_copy(m, h):
        to = dev(right if h == 0 else left, core)
        return remote(mout.at[m % 2, h], fsum.at[m, h], s_mout.at[m % 2, h], s_fsum.at[m, h], to)

    def merge(m):
        slot = m % 3
        wait_bytes(own.at[slot], s_own.at[slot])
        for h in range(2):
            wait_bytes(mg.at[m, h], s_mg.at[m, h])

            @pl.when(m >= 2)
            def _():
                merge_copy(m - 2, h).wait_send()

            @pl.loop(0, half // min(CHUNK, half))
            def _(i):
                size = min(CHUNK, half)
                at = pl.ds(pl.multiple_of(i * size, size), size)
                total = own[slot, h, at].astype(F32) + mg[m, h, 2, at].astype(F32)
                total = total + (mg[m, h, 0, at].astype(F32) + mg[m, h, 1, at].astype(F32))
                mout[m % 2, h, at] = total
            merge_copy(m, h).start()

    def forward_copies(m):
        to = owner_of(m)
        out = []
        for h in range(2):
            at = pl.ds(pl.multiple_of(me * rows + h * half, half), half)
            out.append((fin.at[m, h, 0], xmat.at[at]))
        return to, out

    def finish(m):
        slot = m % 3
        wait_bytes(fin.at[m], s_fin.at[m])
        wait_bytes(momin.at[m % 2], s_mom.at[m % 2])
        size = min(CHUNK, half)
        acc = jnp.zeros((8, 128), F32)
        for h in range(2):
            wait_bytes(fsum.at[m, h], s_fsum.at[m, h])

            def part(i, acc):
                at = pl.ds(pl.multiple_of(i * size, size), size)
                mom_at = pl.ds(pl.multiple_of(h * half + i * size, size), size)
                total = own[slot, 2 + h, at].astype(F32) + fin[m, h, 2, at].astype(F32)
                total = total + (fin[m, h, 0, at].astype(F32) + fin[m, h, 1, at].astype(F32))
                total = total + fsum[m, h, at]
                new = MOMENTUM_COEF * momin[m % 2, mom_at] + total
                fsum[m, h, at] = new
                fin[m, h, 0, at] = new.astype(BF16)
                square = new * new
                for r in range(0, size, 8):
                    for q in range(0, cols, 128):
                        acc = acc + square[r:r + 8, q:q + 128]
                return acc

            acc = lax.fori_loop(0, half // size, part, acc)
            pltpu.make_async_copy(fsum.at[m, h], mom_out.at[m, pl.ds(h * half, half)], s_momout.at[m]).start()
        nsend[m] = acc
        to, copies = forward_copies(m)

        @pl.when(to == me)
        def _():
            for src, dst in copies:
                pltpu.make_async_copy(src, dst, s_x).start()
            pltpu.make_async_copy(nsend.at[m], ninbox.at[me], s_n).start()

        @pl.when(to != me)
        def _():
            for src, dst in copies:
                remote(src, dst, s_xsend.at[m], s_x, to).start()
            remote(nsend.at[m], ninbox.at[me], s_nsend.at[m], s_n, to).start()

    def w_load(m):
        wait_bytes(fsum.at[m], s_momout.at[m])
        for h in range(2):
            pltpu.make_async_copy(w_ref.at[m, pl.ds(h * half, half)], fsum.at[m, h], s_wload.at[m]).start()

    def ns_begin():
        wait_bytes(xmat, s_x)
        wait_bytes(ninbox, s_n)
        total = jnp.sum(ninbox[...], axis=0)
        total = jnp.sum(jnp.sum(total, axis=0, keepdims=True), axis=1, keepdims=True)
        bound = jnp.sqrt(total) + NORM_EPS

        @pl.loop(0, n_rows // CHUNK)
        def _(i):
            at = pl.ds(pl.multiple_of(i * CHUNK, CHUNK), CHUNK)
            xmat[at] = (xmat[at].astype(F32) / bound).astype(BF16)

    def ns_iter():
        wide = min(512, n_rows)

        @pl.loop(0, n_rows // wide)
        def _(j):
            at = pl.ds(pl.multiple_of(j * wide, wide), wide)
            prod = lax.dot_general(xmat[...], xmat[at, :], (((1,), (1,)), ((), ())), preferred_element_type=F32)
            gram[:, at] = prod.astype(BF16)

        @pl.loop(0, n_rows // wide)
        def _(j):
            at = pl.ds(pl.multiple_of(j * wide, wide), wide)
            prod = jnp.dot(gram[...], gram[:, at], preferred_element_type=F32)
            poly[:, at] = (COEF_B * gram[:, at].astype(F32) + COEF_C * prod).astype(BF16)

        wide_x = min(512, cols)

        @pl.loop(0, cols // wide_x)
        def _(j):
            at = pl.ds(pl.multiple_of(j * wide_x, wide_x), wide_x)
            prod = jnp.dot(poly[...], xmat[:, at], preferred_element_type=F32)
            xmat[:, at] = (COEF_A * xmat[:, at].astype(F32) + prod).astype(BF16)

    def iters_done(s):
        early = jnp.clip(ITERS_PER_STEP * (s - my_mat - 2), 0, NS_ITERS)
        return jnp.where(s >= n_mats, NS_ITERS, early)

    barrier = pltpu.get_barrier_semaphore()
    for i in range(1, group):
        pl.semaphore_signal(barrier, inc=1, device_id={"data": (me + i) % group}, device_id_type=MESH)
    pl.semaphore_wait(barrier, group - 1)

    @pl.loop(0, AHEAD)
    def _(m):
        issue_raw(m)
    load_own(0)

    @pl.loop(0, n_mats + 1)
    def _(s):
        @pl.when(s + AHEAD < n_mats)
        def _():
            issue_raw(s + AHEAD)

        @pl.when(s + 1 < n_mats)
        def _():
            load_own(s + 1)

        @pl.when(s < n_mats)
        def _():
            pltpu.make_async_copy(mom_ref.at[s], momin.at[s % 2], s_mom.at[s % 2]).start()
            merge(s)

        @pl.when(s >= 1)
        def _():
            finish(s - 1)

        @pl.when(s >= 2)
        def _():
            w_load(s - 2)

        lo, hi = iters_done(s - 1), iters_done(s)

        @pl.when((lo == 0) & (hi > 0))
        def _():
            ns_begin()

        def run(i, carry):
            ns_iter()
            return carry
        lax.fori_loop(lo, hi, run, 0)

    w_load(n_mats - 1)

    pltpu.make_async_copy(xmat.at[pl.ds(pl.multiple_of(me * rows, rows), rows)], ret.at[my_mat], s_ret.at[my_mat]).start()
    for i in range(1, group):
        to = (me + i) % group
        remote(xmat.at[pl.ds(pl.multiple_of(to * rows, rows), rows)], ret.at[my_mat], s_rsend, s_ret.at[my_mat], to).start()

    @pl.loop(0, n_mats)
    def _(m):
        wait_bytes(ret.at[m], s_ret.at[m])
        wait_bytes(fsum.at[m], s_wload.at[m])
        size = min(CHUNK, half)
        for h in range(2):
            @pl.loop(0, half // size)
            def _(i):
                at = pl.ds(pl.multiple_of(i * size, size), size)
                ret_at = pl.ds(pl.multiple_of(h * half + i * size, size), size)
                w = fsum[m, h, at]
                fsum[m, h, at] = w - LEARN_RATE * (ret[m, ret_at].astype(F32) * scale + WEIGHT_DECAY * w)
            pltpu.make_async_copy(fsum.at[m, h], w_out.at[m, pl.ds(h * half, half)], s_wout.at[m]).start()

    @pl.loop(0, n_mats)
    def _(m):
        done = g_ref.at[0, m, pl.ds(0, 12 * half)]
        wait_bytes(done, s_gsend.at[m])
        wait_bytes(fsum.at[m], s_wout.at[m])

        @pl.when(owner_of(m) != me)
        def _():
            wait_bytes(ret.at[m], s_xsend.at[m])
            wait_bytes(nsend.at[m], s_nsend.at[m])
    for m in range(n_mats - 2, n_mats):
        for h in range(2):
            merge_copy(m, h).wait_send()
    wait_bytes(xmat.at[pl.ds(0, (group - 1) * rows)], s_rsend)


def solution(mesh):
    group = mesh.shape['data']
    row_spec = P('stage', 'data', None)
    grad_spec = P(('stage', 'data'), None, None, None)

    def local_step(w_rows, mom_rows, grad_full):
        n_mats, rows, cols = w_rows.shape
        half = rows // 2
        n_rows = rows * group
        scale = 0.2 * math.sqrt(max(n_rows, cols))
        hbm = pl.BlockSpec(memory_space=pl.ANY)
        dma = pltpu.SemaphoreType.DMA
        flops = NS_ITERS * (4 * n_rows * n_rows * cols + 2 * n_rows ** 3)
        return pl.pallas_call(
            functools.partial(fused_kernel, group, scale),
            out_shape=(jax.ShapeDtypeStruct(w_rows.shape, F32), jax.ShapeDtypeStruct(w_rows.shape, F32)),
            in_specs=[hbm] * 3,
            out_specs=(hbm, hbm),
            scratch_shapes=[
                pltpu.VMEM((n_mats, 2, 3, half, cols), BF16),
                pltpu.VMEM((n_mats, 2, 3, half, cols), BF16),
                pltpu.VMEM((n_mats, 2, half, cols), F32),
                pltpu.VMEM((3, 4, half, cols), BF16),
                pltpu.VMEM((2, 2, half, cols), F32),
                pltpu.VMEM((2, rows, cols), F32),
                pltpu.VMEM((n_rows, cols), BF16),
                pltpu.VMEM((n_rows, n_rows), BF16),
                pltpu.VMEM((n_rows, n_rows), BF16),
                pltpu.VMEM((n_mats, rows, cols), BF16),
                pltpu.VMEM((n_mats, 8, 128), F32),
                pltpu.VMEM((group, 8, 128), F32),
                dma((n_mats, 2)), dma((n_mats,)), dma((n_mats, 2)), dma((3,)), dma((2, 2)), dma((2,)),
                dma, dma, dma((n_mats,)),
                dma((n_mats,)), dma((n_mats,)), dma((n_mats,)), dma, dma((n_mats,)), dma((n_mats,)), dma((n_mats,)),
            ],
            compiler_params=pltpu.CompilerParams(collective_id=0, has_side_effects=True, vmem_limit_bytes=67043328),
            cost_estimate=pl.CostEstimate(flops=flops, bytes_accessed=2 ** 26, transcendentals=0),
            name="muon_step",
        )(w_rows, mom_rows, grad_full)

    return jax.shard_map(local_step, mesh=mesh, in_specs=(row_spec, row_spec, grad_spec), out_specs=(row_spec, row_spec), check_vma=False)
```

```python
import functools
import math
import jax
import jax.numpy as jnp
from jax import lax
from jax.experimental import pallas as pl
from jax.experimental.pallas import tpu as pltpu
from jax.sharding import PartitionSpec as P

MOMENTUM_COEF = 0.95
LEARN_RATE = 0.05
WEIGHT_DECAY = 0.2
NORM_EPS = 1e-7
COEF_A = 3.4445
COEF_B = -4.7750
COEF_C = 2.0315
NS_ITERS = 5

CORES = 2
AHEAD = 2
CHUNK = 32
ITERS_PER_STEP = 2
XWIDE = 512
HOLD = 2
MESH = pl.DeviceIdType.MESH
F32 = jnp.float32
BF16 = jnp.bfloat16


def fused_kernel(group, scale, w_ref, mom_ref, g_ref, w_out, mom_out,
                 mg, fin, fsum, own, mout, momin, xin, xbuf, row, colo, poly, ret, nsend, ninbox,
                 s_mg, s_fin, s_fsum, s_own, s_mout, s_mom, s_x, s_n, s_ret,
                 s_gsend, s_xsend, s_nsend, s_rsend, s_momout, s_wload, s_wout,
                 s_xp, s_xps, s_ap, s_aps):
    n_mats, rows, cols = w_ref.shape
    half = rows // 2
    chips = group // CORES
    hr = rows * chips
    me = lax.axis_index("data")
    chip, core = me // CORES, me % CORES
    right, left, far = (chip + 1) % chips, (chip + chips - 1) % chips, (chip + 2) % chips

    def dev(a_chip, a_core):
        return a_chip * CORES + a_core

    mate = dev(chip, 1 - core)

    def owner_chip(m):
        return jnp.where(m < chips, m, 2 * chips - 1 - m)

    def my_mat(e):
        return jnp.where(e == 0, chip, 2 * chips - 1 - chip)

    def grad_rows(m, a_chip, a_core, h):
        start = pl.multiple_of(dev(a_chip, a_core) * rows + h * half, half)
        return g_ref.at[0, m, pl.ds(start, half)]

    def remote(src, dst, send, recv, to):
        return pltpu.make_async_remote_copy(src_ref=src, dst_ref=dst, send_sem=send, recv_sem=recv,
                                            device_id={"data": to}, device_id_type=MESH)

    def wait_bytes(ref, sem, name=None):
        if name is None:
            pltpu.make_async_copy(ref, ref, sem).wait()
        else:
            with jax.named_scope(name):
                pltpu.make_async_copy(ref, ref, sem).wait()

    def issue_raw(m):
        send = s_gsend.at[m]
        for kk in range(CORES):
            remote(grad_rows(m, far, kk, 0), mg.at[m, 0, core], send, s_mg.at[m, 0], dev(right, kk)).start()
            remote(grad_rows(m, far, kk, 1), mg.at[m, 1, core], send, s_mg.at[m, 1], dev(left, kk)).start()
        remote(grad_rows(m, right, 1 - core, 0), mg.at[m, 0, 2], send, s_mg.at[m, 0], mate).start()
        remote(grad_rows(m, left, 1 - core, 1), mg.at[m, 1, 2], send, s_mg.at[m, 1], mate).start()
        for kk in range(CORES):
            remote(grad_rows(m, right, kk, 1), fin.at[m, 1, core], send, s_fin.at[m], dev(right, kk)).start()
            remote(grad_rows(m, left, kk, 0), fin.at[m, 0, core], send, s_fin.at[m], dev(left, kk)).start()
        for h in range(2):
            remote(grad_rows(m, chip, 1 - core, h), fin.at[m, h, 2], send, s_fin.at[m], mate).start()

    def load_own(m):
        slot = m % 3
        pltpu.make_async_copy(grad_rows(m, right, core, 0), own.at[slot, 0], s_own.at[slot]).start()
        pltpu.make_async_copy(grad_rows(m, left, core, 1), own.at[slot, 1], s_own.at[slot]).start()
        for h in range(2):
            pltpu.make_async_copy(grad_rows(m, chip, core, h), own.at[slot, 2 + h], s_own.at[slot]).start()

    def merge_copy(m, h):
        to = dev(right if h == 0 else left, core)
        return remote(mout.at[m % 2, h], fsum.at[m, h], s_mout.at[m % 2, h], s_fsum.at[m, h], to)

    def merge(m):
        slot = m % 3
        wait_bytes(own.at[slot], s_own.at[slot])
        for h in range(2):
            wait_bytes(mg.at[m, h], s_mg.at[m, h], "wait_mg")

            @pl.when(m >= 2)
            def _():
                merge_copy(m - 2, h).wait_send()

            @pl.loop(0, half // min(CHUNK, half))
            def _(i):
                size = min(CHUNK, half)
                at = pl.ds(pl.multiple_of(i * size, size), size)
                total = own[slot, h, at].astype(F32) + mg[m, h, 2, at].astype(F32)
                total = total + (mg[m, h, 0, at].astype(F32) + mg[m, h, 1, at].astype(F32))
                mout[m % 2, h, at] = total
            merge_copy(m, h).start()

    def finish(m):
        slot = m % 3
        oc = owner_chip(m)
        late = m // chips
        wait_bytes(fin.at[m], s_fin.at[m])
        wait_bytes(momin.at[m % 2], s_mom.at[m % 2])
        size = min(CHUNK, half)
        acc = jnp.zeros((8, 128), F32)
        for h in range(2):
            wait_bytes(fsum.at[m, h], s_fsum.at[m, h], "wait_fsum")

            def part(i, acc):
                at = pl.ds(pl.multiple_of(i * size, size), size)
                mom_at = pl.ds(pl.multiple_of(h * half + i * size, size), size)
                total = own[slot, 2 + h, at].astype(F32) + fin[m, h, 2, at].astype(F32)
                total = total + (fin[m, h, 0, at].astype(F32) + fin[m, h, 1, at].astype(F32))
                total = total + fsum[m, h, at]
                new = MOMENTUM_COEF * momin[m % 2, mom_at] + total
                fsum[m, h, at] = new
                fin[m, h, 0, at] = new.astype(BF16)
                square = new * new
                for r in range(0, size, 8):
                    for q in range(0, cols, 128):
                        acc = acc + square[r:r + 8, q:q + 128]
                return acc

            acc = lax.fori_loop(0, half // size, part, acc)
            src = fin.at[m, h, 0]
            dst = xin.at[late, pl.ds(pl.multiple_of(chip * rows + h * half, half), half)]

            @pl.when(oc == chip)
            def _():
                pltpu.make_async_copy(src, dst, s_x.at[late]).start()

            @pl.when(oc != chip)
            def _():
                remote(src, dst, s_xsend.at[m], s_x.at[late], dev(oc, core)).start()
            pltpu.make_async_copy(fsum.at[m, h], mom_out.at[m, pl.ds(h * half, half)], s_momout.at[m]).start()
        nsend[m] = acc
        sum_to = ninbox.at[late, me]

        @pl.when(oc == chip)
        def _():
            pltpu.make_async_copy(nsend.at[m], sum_to, s_n.at[late]).start()
            remote(nsend.at[m], sum_to, s_nsend.at[m], s_n.at[late], mate).start()

        @pl.when(oc != chip)
        def _():
            for kk in range(CORES):
                remote(nsend.at[m], sum_to, s_nsend.at[m], s_n.at[late], dev(oc, kk)).start()

    def w_load(m):
        wait_bytes(fsum.at[m], s_momout.at[m])
        for h in range(2):
            pltpu.make_async_copy(w_ref.at[m, pl.ds(h * half, half)], fsum.at[m, h], s_wload.at[m]).start()

    def to_mate(g, par, at):
        return remote(xbuf.at[par, pl.ds(0, hr), at], xbuf.at[par, pl.ds(hr, hr), at], s_xps.at[g], s_xp.at[g], mate)

    def ns_begin(e):
        g, par = e * NS_ITERS, (e * NS_ITERS) % 2
        wait_bytes(xin.at[e], s_x.at[e], "wait_x")
        wait_bytes(ninbox.at[e], s_n.at[e], "wait_n")
        total = jnp.sum(ninbox[e], axis=0)
        total = jnp.sum(jnp.sum(total, axis=0, keepdims=True), axis=1, keepdims=True)
        bound = jnp.sqrt(total) + NORM_EPS

        @pl.loop(0, chips)
        def _(b):
            @pl.loop(0, rows // CHUNK)
            def _(i):
                at = pl.ds(pl.multiple_of(b * rows + i * CHUNK, CHUNK), CHUNK)
                xbuf[par, at] = (xin[e, at].astype(F32) / bound).astype(BF16)
            at = pl.ds(pl.multiple_of(b * rows, rows), rows)
            there = pl.ds(pl.multiple_of(hr + b * rows, rows), rows)
            remote(xbuf.at[par, at], xbuf.at[par, there], s_xps.at[g], s_xp.at[g], mate).start()

    def ns_iter(g):
        e, i, par = g // NS_ITERS, g % NS_ITERS, g % 2
        nxt = 1 - par
        first, second = pl.ds(0, hr), pl.ds(hr, hr)
        transposed = (((1,), (1,)), ((), ()))
        diag = remote(row.at[:, first], colo.at[par, second], s_aps.at[g], s_ap.at[g], mate)

        with jax.named_scope("gram"):
            prod = lax.dot_general(xbuf[par, first], xbuf[par, first], transposed, preferred_element_type=F32)
            row[:, first] = prod.astype(BF16)
            diag.start()
        wait_bytes(xbuf.at[par, second], s_xp.at[g], "wait_xp")
        with jax.named_scope("gram2"):
            prod = lax.dot_general(xbuf[par, first], xbuf[par, second], transposed, preferred_element_type=F32)
            prod = prod.astype(BF16)
            row[:, second] = prod
            colo[par, first] = prod
        with jax.named_scope("sq1"):
            prod = lax.dot_general(row[...], row[...], transposed, preferred_element_type=F32)
            poly[:, first] = (COEF_B * row[:, first].astype(F32) + COEF_C * prod).astype(BF16)
        wait_bytes(colo.at[par, second], s_ap.at[g], "wait_ap")
        with jax.named_scope("sq2"):
            prod = jnp.dot(row[...], colo[par], preferred_element_type=F32)
            poly[:, second] = (COEF_B * row[:, second].astype(F32) + COEF_C * prod).astype(BF16)
        wide = min(XWIDE, cols)

        with jax.named_scope("newx"):
            @pl.loop(0, cols // wide)
            def _(j):
                at = pl.ds(pl.multiple_of(j * wide, wide), wide)
                prod = jnp.dot(poly[...], xbuf[par, :, at], preferred_element_type=F32)
                new = (COEF_A * xbuf[par, first, at].astype(F32) + prod).astype(BF16)

                @pl.when(i < NS_ITERS - 1)
                def _():
                    xbuf[nxt, first, at] = new
                    to_mate(g + 1, nxt, at).start()

                @pl.when(i == NS_ITERS - 1)
                def _():
                    xin[e, :, at] = new
        diag.wait_send()
        wait_bytes(xbuf.at[par, first], s_xps.at[g])

    def give_back(e):
        for c in range(chips):
            block = xin.at[e, pl.ds(c * rows, rows)]
            mat = my_mat(e)

            @pl.when(chip == c)
            def _():
                pltpu.make_async_copy(block, ret.at[mat], s_ret.at[mat]).start()

            @pl.when(chip != c)
            def _():
                remote(block, ret.at[mat], s_rsend.at[e], s_ret.at[mat], dev(c, core)).start()

    def early_done(s):
        return jnp.clip(ITERS_PER_STEP * (s - chip - 2), 0, NS_ITERS)

    barrier = pltpu.get_barrier_semaphore()
    for i in range(1, group):
        pl.semaphore_signal(barrier, inc=1, device_id={"data": (me + i) % group}, device_id_type=MESH)
    pl.semaphore_wait(barrier, group - 1)

    @pl.loop(0, AHEAD)
    def _(m):
        issue_raw(m)
    load_own(0)

    @pl.loop(0, n_mats + 2)
    def _(s):
        @pl.when(s + AHEAD < n_mats)
        def _():
            issue_raw(s + AHEAD)

        @pl.when(s + 1 < n_mats)
        def _():
            load_own(s + 1)

        @pl.when(s < n_mats)
        def _():
            pltpu.make_async_copy(mom_ref.at[s], momin.at[s % 2], s_mom.at[s % 2]).start()
            merge(s)

        last = s == n_mats + 1
        lo = jnp.where(s >= n_mats, early_done(n_mats - 1), early_done(s - 1))
        hi = jnp.where(last, 2 * NS_ITERS, jnp.where(s >= n_mats, lo, early_done(s)))

        def run(g, carry):
            @pl.when(g % NS_ITERS == 0)
            def _():
                ns_begin(g // NS_ITERS)

            @pl.when(g == jnp.where(chip == 0, NS_ITERS, NS_ITERS + HOLD))
            def _():
                give_back(0)
            ns_iter(g)
            return carry
        lax.fori_loop(lo, hi, run, 0)

        @pl.when((s >= 1) & (s <= n_mats))
        def _():
            finish(s - 1)

        @pl.when(s >= 2)
        def _():
            w_load(s - 2)

    give_back(1)

    @pl.loop(0, n_mats)
    def _(m):
        wait_bytes(ret.at[m], s_ret.at[m], "wait_ret")
        wait_bytes(fsum.at[m], s_wload.at[m])
        size = min(CHUNK, half)
        for h in range(2):
            @pl.loop(0, half // size)
            def _(i):
                at = pl.ds(pl.multiple_of(i * size, size), size)
                ret_at = pl.ds(pl.multiple_of(h * half + i * size, size), size)
                w = fsum[m, h, at]
                fsum[m, h, at] = w - LEARN_RATE * (ret[m, ret_at].astype(F32) * scale + WEIGHT_DECAY * w)
            pltpu.make_async_copy(fsum.at[m, h], w_out.at[m, pl.ds(h * half, half)], s_wout.at[m]).start()

    @pl.loop(0, n_mats)
    def _(m):
        done = g_ref.at[0, m, pl.ds(0, 12 * half)]
        wait_bytes(done, s_gsend.at[m])
        wait_bytes(fsum.at[m], s_wout.at[m])

        @pl.when(owner_chip(m) == chip)
        def _():
            wait_bytes(nsend.at[0], s_nsend.at[m])

        @pl.when(owner_chip(m) != chip)
        def _():
            wait_bytes(ret.at[m], s_xsend.at[m])
            wait_bytes(nsend.at[pl.ds(0, CORES)], s_nsend.at[m])
    for m in range(n_mats - 2, n_mats):
        for h in range(2):
            merge_copy(m, h).wait_send()
    for e in range(2):
        wait_bytes(xin.at[e, pl.ds(0, (chips - 1) * rows)], s_rsend.at[e])


def solution(mesh):
    group = mesh.shape['data']
    row_spec = P('stage', 'data', None)
    grad_spec = P(('stage', 'data'), None, None, None)

    def local_step(w_rows, mom_rows, grad_full):
        n_mats, rows, cols = w_rows.shape
        half = rows // 2
        n_rows = rows * group
        hr = n_rows // CORES
        scale = 0.2 * math.sqrt(max(n_rows, cols))
        hbm = pl.BlockSpec(memory_space=pl.ANY)
        dma = pltpu.SemaphoreType.DMA
        flops = NS_ITERS * (4 * n_rows * n_rows * cols + 2 * n_rows ** 3)
        return pl.pallas_call(
            functools.partial(fused_kernel, group, scale),
            out_shape=(jax.ShapeDtypeStruct(w_rows.shape, F32), jax.ShapeDtypeStruct(w_rows.shape, F32)),
            in_specs=[hbm] * 3,
            out_specs=(hbm, hbm),
            scratch_shapes=[
                pltpu.VMEM((n_mats, 2, 3, half, cols), BF16),
                pltpu.VMEM((n_mats, 2, 3, half, cols), BF16),
                pltpu.VMEM((n_mats, 2, half, cols), F32),
                pltpu.VMEM((3, 4, half, cols), BF16),
                pltpu.VMEM((2, 2, half, cols), F32),
                pltpu.VMEM((2, rows, cols), F32),
                pltpu.VMEM((2, hr, cols), BF16),
                pltpu.VMEM((2, n_rows, cols), BF16),
                pltpu.VMEM((hr, n_rows), BF16),
                pltpu.VMEM((2, n_rows, hr), BF16),
                pltpu.VMEM((hr, n_rows), BF16),
                pltpu.VMEM((n_mats, rows, cols), BF16),
                pltpu.VMEM((n_mats, 8, 128), F32),
                pltpu.VMEM((2, group, 8, 128), F32),
                dma((n_mats, 2)), dma((n_mats,)), dma((n_mats, 2)), dma((3,)), dma((2, 2)), dma((2,)),
                dma((2,)), dma((2,)), dma((n_mats,)),
                dma((n_mats,)), dma((n_mats,)), dma((n_mats,)), dma((2,)), dma((n_mats,)), dma((n_mats,)), dma((n_mats,)),
                dma((2 * NS_ITERS,)), dma((2 * NS_ITERS,)), dma((2 * NS_ITERS,)), dma((2 * NS_ITERS,)),
            ],
            compiler_params=pltpu.CompilerParams(collective_id=0, has_side_effects=True, vmem_limit_bytes=67043328),
            cost_estimate=pl.CostEstimate(flops=flops, bytes_accessed=2 ** 26, transcendentals=0),
            name="muon_step",
        )(w_rows, mom_rows, grad_full)

    return jax.shard_map(local_step, mesh=mesh, in_specs=(row_spec, row_spec, grad_spec), out_specs=(row_spec, row_spec), check_vma=False)
```

```python
import functools
import math
import jax
import jax.numpy as jnp
from jax import lax
from jax.experimental import pallas as pl
from jax.experimental.pallas import tpu as pltpu
from jax.sharding import PartitionSpec as P

MOMENTUM_COEF = 0.95
LEARN_RATE = 0.05
WEIGHT_DECAY = 0.2
NORM_EPS = 1e-7
COEF_A = 3.4445
COEF_B = -4.7750
COEF_C = 2.0315
NS_ITERS = 5

CORES = 2
AHEAD = 2
CHUNK = 32
ITERS_PER_STEP = 2
HOLD = 1
MESH = pl.DeviceIdType.MESH
F32 = jnp.float32
BF16 = jnp.bfloat16


def x_parts(cols):
    parts = (cols // 2, cols // 4, cols // 4)
    return [(sum(parts[:i]), width) for i, width in enumerate(parts)]


def fused_kernel(group, scale, w_ref, mom_ref, g_ref, w_out, mom_out,
                 mg, fin, fsum, own, mout, momin, xin, xbuf, row, colo, poly, ret, nsend, ninbox,
                 s_mg, s_fin, s_fsum, s_own, s_mout, s_mom, s_x, s_n, s_ret,
                 s_gsend, s_xsend, s_nsend, s_rsend, s_momout, s_wload, s_wout,
                 s_xp, s_xps, s_ap, s_aps, s_keep):
    n_mats, rows, cols = w_ref.shape
    half = rows // 2
    chips = group // CORES
    hr = rows * chips
    me = lax.axis_index("data")
    chip, core = me // CORES, me % CORES
    right, left, far = (chip + 1) % chips, (chip + chips - 1) % chips, (chip + 2) % chips

    def dev(a_chip, a_core):
        return a_chip * CORES + a_core

    mate = dev(chip, 1 - core)

    def owner_chip(m):
        return jnp.where(m < chips, m, 2 * chips - 1 - m)

    def my_mat(e):
        return jnp.where(e == 0, chip, 2 * chips - 1 - chip)

    def grad_rows(m, a_chip, a_core, h):
        start = pl.multiple_of(dev(a_chip, a_core) * rows + h * half, half)
        return g_ref.at[0, m, pl.ds(start, half)]

    def remote(src, dst, send, recv, to):
        return pltpu.make_async_remote_copy(src_ref=src, dst_ref=dst, send_sem=send, recv_sem=recv,
                                            device_id={"data": to}, device_id_type=MESH)

    def wait_bytes(ref, sem, name=None):
        if name is None:
            pltpu.make_async_copy(ref, ref, sem).wait()
        else:
            with jax.named_scope(name):
                pltpu.make_async_copy(ref, ref, sem).wait()

    def issue_raw(m):
        send = s_gsend.at[m]
        for kk in range(CORES):
            remote(grad_rows(m, far, kk, 0), mg.at[m, 0, core], send, s_mg.at[m, 0], dev(right, kk)).start()
            remote(grad_rows(m, far, kk, 1), mg.at[m, 1, core], send, s_mg.at[m, 1], dev(left, kk)).start()
        remote(grad_rows(m, right, 1 - core, 0), mg.at[m, 0, 2], send, s_mg.at[m, 0], mate).start()
        remote(grad_rows(m, left, 1 - core, 1), mg.at[m, 1, 2], send, s_mg.at[m, 1], mate).start()
        for kk in range(CORES):
            remote(grad_rows(m, right, kk, 1), fin.at[m, 1, core], send, s_fin.at[m], dev(right, kk)).start()
            remote(grad_rows(m, left, kk, 0), fin.at[m, 0, core], send, s_fin.at[m], dev(left, kk)).start()
        for h in range(2):
            remote(grad_rows(m, chip, 1 - core, h), fin.at[m, h, 2], send, s_fin.at[m], mate).start()

    def load_own(m):
        slot = m % 3
        pltpu.make_async_copy(grad_rows(m, right, core, 0), own.at[slot, 0], s_own.at[slot]).start()
        pltpu.make_async_copy(grad_rows(m, left, core, 1), own.at[slot, 1], s_own.at[slot]).start()
        for h in range(2):
            pltpu.make_async_copy(grad_rows(m, chip, core, h), own.at[slot, 2 + h], s_own.at[slot]).start()

    def merge_copy(m, h):
        to = dev(right if h == 0 else left, core)
        return remote(mout.at[m % 2, h], fsum.at[m, h], s_mout.at[m % 2, h], s_fsum.at[m, h], to)

    def merge(m):
        slot = m % 3
        wait_bytes(own.at[slot], s_own.at[slot])
        for h in range(2):
            wait_bytes(mg.at[m, h], s_mg.at[m, h], "wait_mg")

            @pl.when(m >= 2)
            def _():
                merge_copy(m - 2, h).wait_send()

            @pl.loop(0, half // min(CHUNK, half))
            def _(i):
                size = min(CHUNK, half)
                at = pl.ds(pl.multiple_of(i * size, size), size)
                total = own[slot, h, at].astype(F32) + mg[m, h, 2, at].astype(F32)
                total = total + (mg[m, h, 0, at].astype(F32) + mg[m, h, 1, at].astype(F32))
                mout[m % 2, h, at] = total
            merge_copy(m, h).start()

    def forward(m, h):
        oc = owner_chip(m)
        late = m // chips
        src = fin.at[m, h, 0]
        dst = xin.at[late, pl.ds(pl.multiple_of(chip * rows + h * half, half), half)]

        @pl.when(oc == chip)
        def _():
            pltpu.make_async_copy(src, dst, s_x.at[late]).start()

        @pl.when(oc != chip)
        def _():
            remote(src, dst, s_xsend.at[m], s_x.at[late], dev(oc, core)).start()

    def finish(m):
        slot = m % 3
        oc = owner_chip(m)
        late = m // chips
        wait_bytes(fin.at[m], s_fin.at[m])
        wait_bytes(momin.at[m % 2], s_mom.at[m % 2])
        size = min(CHUNK, half)
        acc = jnp.zeros((8, 128), F32)
        for h in range(2):
            wait_bytes(fsum.at[m, h], s_fsum.at[m, h], "wait_fsum")

            def part(i, acc):
                at = pl.ds(pl.multiple_of(i * size, size), size)
                mom_at = pl.ds(pl.multiple_of(h * half + i * size, size), size)
                total = own[slot, 2 + h, at].astype(F32) + fin[m, h, 2, at].astype(F32)
                total = total + (fin[m, h, 0, at].astype(F32) + fin[m, h, 1, at].astype(F32))
                total = total + fsum[m, h, at]
                new = MOMENTUM_COEF * momin[m % 2, mom_at] + total
                fsum[m, h, at] = new
                fin[m, h, 0, at] = new.astype(BF16)
                square = new * new
                for r in range(0, size, 8):
                    for q in range(0, cols, 128):
                        acc = acc + square[r:r + 8, q:q + 128]
                return acc

            acc = lax.fori_loop(0, half // size, part, acc)

            @pl.when((late == 0) | (m == n_mats - 1))
            def _():
                forward(m, h)
            pltpu.make_async_copy(fsum.at[m, h], mom_out.at[m, pl.ds(h * half, half)], s_momout.at[m]).start()
        nsend[m] = acc
        sum_to = ninbox.at[late, me]

        @pl.when(oc == chip)
        def _():
            pltpu.make_async_copy(nsend.at[m], sum_to, s_n.at[late]).start()
            remote(nsend.at[m], sum_to, s_nsend.at[m], s_n.at[late], mate).start()

        @pl.when(oc != chip)
        def _():
            for kk in range(CORES):
                remote(nsend.at[m], sum_to, s_nsend.at[m], s_n.at[late], dev(oc, kk)).start()

    def w_load(m):
        wait_bytes(fsum.at[m], s_momout.at[m])
        for h in range(2):
            pltpu.make_async_copy(w_ref.at[m, pl.ds(h * half, half)], fsum.at[m, h], s_wload.at[m]).start()

    def to_mate(g, par, at):
        return remote(xbuf.at[par, pl.ds(0, hr), at], xbuf.at[par, pl.ds(hr, hr), at], s_xps.at[g], s_xp.at[g], mate)

    def ns_begin(e):
        g, par = e * NS_ITERS, (e * NS_ITERS) % 2
        wait_bytes(xin.at[e], s_x.at[e], "wait_x")
        wait_bytes(ninbox.at[e], s_n.at[e], "wait_n")
        total = jnp.sum(ninbox[e], axis=0)
        total = jnp.sum(jnp.sum(total, axis=0, keepdims=True), axis=1, keepdims=True)
        bound = jnp.sqrt(total) + NORM_EPS

        @pl.loop(0, chips)
        def _(b):
            @pl.loop(0, rows // CHUNK)
            def _(i):
                at = pl.ds(pl.multiple_of(b * rows + i * CHUNK, CHUNK), CHUNK)
                xbuf[par, at] = (xin[e, at].astype(F32) / bound).astype(BF16)
            at = pl.ds(pl.multiple_of(b * rows, rows), rows)
            there = pl.ds(pl.multiple_of(hr + b * rows, rows), rows)
            remote(xbuf.at[par, at], xbuf.at[par, there], s_xps.at[g], s_xp.at[g], mate).start()

    def ns_iter(g):
        e, i, par = g // NS_ITERS, g % NS_ITERS, g % 2
        nxt = 1 - par
        first, second = pl.ds(0, hr), pl.ds(hr, hr)
        transposed = (((1,), (1,)), ((), ()))
        diag = remote(row.at[:, first], colo.at[par, second], s_aps.at[g], s_ap.at[g], mate)

        with jax.named_scope("gram"):
            prod = lax.dot_general(xbuf[par, first], xbuf[par, first], transposed, preferred_element_type=F32)
            row[:, first] = prod.astype(BF16)
            diag.start()
        wait_bytes(xbuf.at[par, second], s_xp.at[g], "wait_xp")
        with jax.named_scope("gram2"):
            prod = lax.dot_general(xbuf[par, first], xbuf[par, second], transposed, preferred_element_type=F32)
            prod = prod.astype(BF16)
            row[:, second] = prod
            colo[par, first] = prod
        with jax.named_scope("sq1"):
            prod = lax.dot_general(row[...], row[...], transposed, preferred_element_type=F32)
            poly[:, first] = (COEF_B * row[:, first].astype(F32) + COEF_C * prod).astype(BF16)
        wait_bytes(colo.at[par, second], s_ap.at[g], "wait_ap")
        with jax.named_scope("sq2"):
            prod = jnp.dot(row[...], colo[par], preferred_element_type=F32)
            poly[:, second] = (COEF_B * row[:, second].astype(F32) + COEF_C * prod).astype(BF16)
        with jax.named_scope("newx"):
            for lo, wide in x_parts(cols):
                at = pl.ds(lo, wide)
                prod = jnp.dot(poly[...], xbuf[par, :, at], preferred_element_type=F32)
                xbuf[nxt, first, at] = (COEF_A * xbuf[par, first, at].astype(F32) + prod).astype(BF16)

                @pl.when(i < NS_ITERS - 1)
                def _():
                    to_mate(g + 1, nxt, at).start()

                @pl.when(g == 2 * NS_ITERS - 1)
                def _():
                    give_back(1, xbuf.at[nxt], at)

        @pl.when(g == NS_ITERS - 1)
        def _():
            keep = pltpu.make_async_copy(xbuf.at[nxt, first], xin.at[0], s_keep)
            keep.start()
            keep.wait()
        diag.wait_send()
        wait_bytes(xbuf.at[par, first], s_xps.at[g])

    def give_back(e, src, at):
        mat = my_mat(e)
        dst = ret.at[mat, :, at]
        for c in range(chips):
            block = src.at[pl.ds(c * rows, rows), at]

            @pl.when(chip == c)
            def _():
                pltpu.make_async_copy(block, dst, s_ret.at[mat]).start()

            @pl.when(chip != c)
            def _():
                remote(block, dst, s_rsend.at[e], s_ret.at[mat], dev(c, core)).start()

    def early_done(s):
        return jnp.clip(ITERS_PER_STEP * (s - chip - 2), 0, NS_ITERS)

    barrier = pltpu.get_barrier_semaphore()
    for i in range(1, group):
        pl.semaphore_signal(barrier, inc=1, device_id={"data": (me + i) % group}, device_id_type=MESH)
    pl.semaphore_wait(barrier, group - 1)

    @pl.loop(0, AHEAD)
    def _(m):
        issue_raw(m)
    load_own(0)

    @pl.loop(0, n_mats + 2)
    def _(s):
        @pl.when(s + AHEAD < n_mats)
        def _():
            issue_raw(s + AHEAD)

        @pl.when(s + 1 < n_mats)
        def _():
            load_own(s + 1)

        @pl.when(s < n_mats)
        def _():
            pltpu.make_async_copy(mom_ref.at[s], momin.at[s % 2], s_mom.at[s % 2]).start()
            merge(s)

        @pl.when(s == n_mats - 1)
        def _():
            @pl.loop(chips, n_mats - 2)
            def _(m):
                for h in range(2):
                    forward(m, h)

        last = s == n_mats + 1
        lo = jnp.where(s >= n_mats, early_done(n_mats - 1), early_done(s - 1))
        hi = jnp.where(last, 2 * NS_ITERS, jnp.where(s >= n_mats, lo, early_done(s)))

        def run(g, carry):
            @pl.when(g % NS_ITERS == 0)
            def _():
                ns_begin(g // NS_ITERS)

            @pl.when(g == NS_ITERS + HOLD)
            def _():
                give_back(0, xin.at[0], pl.ds(0, cols))
            ns_iter(g)
            return carry
        lax.fori_loop(lo, hi, run, 0)

        @pl.when((s >= 1) & (s <= n_mats))
        def _():
            finish(s - 1)

        @pl.when(s == n_mats - 1)
        def _():
            for h in range(2):
                forward(n_mats - 2, h)

        @pl.when(s >= 2)
        def _():
            w_load(s - 2)

    @pl.loop(0, n_mats)
    def _(m):
        wait_bytes(ret.at[m], s_ret.at[m], "wait_ret")
        wait_bytes(fsum.at[m], s_wload.at[m])
        size = min(CHUNK, half)
        for h in range(2):
            @pl.loop(0, half // size)
            def _(i):
                at = pl.ds(pl.multiple_of(i * size, size), size)
                ret_at = pl.ds(pl.multiple_of(h * half + i * size, size), size)
                w = fsum[m, h, at]
                fsum[m, h, at] = w - LEARN_RATE * (ret[m, ret_at].astype(F32) * scale + WEIGHT_DECAY * w)
            pltpu.make_async_copy(fsum.at[m, h], w_out.at[m, pl.ds(h * half, half)], s_wout.at[m]).start()

    @pl.loop(0, n_mats)
    def _(m):
        done = g_ref.at[0, m, pl.ds(0, 12 * half)]
        wait_bytes(done, s_gsend.at[m])
        wait_bytes(fsum.at[m], s_wout.at[m])

        @pl.when(owner_chip(m) == chip)
        def _():
            wait_bytes(nsend.at[0], s_nsend.at[m])

        @pl.when(owner_chip(m) != chip)
        def _():
            wait_bytes(ret.at[m], s_xsend.at[m])
            wait_bytes(nsend.at[pl.ds(0, CORES)], s_nsend.at[m])
    for m in range(n_mats - 2, n_mats):
        for h in range(2):
            merge_copy(m, h).wait_send()
    for e in range(2):
        wait_bytes(xin.at[e, pl.ds(0, (chips - 1) * rows)], s_rsend.at[e])


def solution(mesh):
    group = mesh.shape['data']
    row_spec = P('stage', 'data', None)
    grad_spec = P(('stage', 'data'), None, None, None)

    def local_step(w_rows, mom_rows, grad_full):
        n_mats, rows, cols = w_rows.shape
        half = rows // 2
        n_rows = rows * group
        hr = n_rows // CORES
        scale = 0.2 * math.sqrt(max(n_rows, cols))
        hbm = pl.BlockSpec(memory_space=pl.ANY)
        dma = pltpu.SemaphoreType.DMA
        flops = NS_ITERS * (4 * n_rows * n_rows * cols + 2 * n_rows ** 3)
        return pl.pallas_call(
            functools.partial(fused_kernel, group, scale),
            out_shape=(jax.ShapeDtypeStruct(w_rows.shape, F32), jax.ShapeDtypeStruct(w_rows.shape, F32)),
            in_specs=[hbm] * 3,
            out_specs=(hbm, hbm),
            scratch_shapes=[
                pltpu.VMEM((n_mats, 2, 3, half, cols), BF16),
                pltpu.VMEM((n_mats, 2, 3, half, cols), BF16),
                pltpu.VMEM((n_mats, 2, half, cols), F32),
                pltpu.VMEM((3, 4, half, cols), BF16),
                pltpu.VMEM((2, 2, half, cols), F32),
                pltpu.VMEM((2, rows, cols), F32),
                pltpu.VMEM((2, hr, cols), BF16),
                pltpu.VMEM((2, n_rows, cols), BF16),
                pltpu.VMEM((hr, n_rows), BF16),
                pltpu.VMEM((2, n_rows, hr), BF16),
                pltpu.VMEM((hr, n_rows), BF16),
                pltpu.VMEM((n_mats, rows, cols), BF16),
                pltpu.VMEM((n_mats, 8, 128), F32),
                pltpu.VMEM((2, group, 8, 128), F32),
                dma((n_mats, 2)), dma((n_mats,)), dma((n_mats, 2)), dma((3,)), dma((2, 2)), dma((2,)),
                dma((2,)), dma((2,)), dma((n_mats,)),
                dma((n_mats,)), dma((n_mats,)), dma((n_mats,)), dma((2,)), dma((n_mats,)), dma((n_mats,)), dma((n_mats,)),
                dma((2 * NS_ITERS,)), dma((2 * NS_ITERS,)), dma((2 * NS_ITERS,)), dma((2 * NS_ITERS,)), dma,
            ],
            compiler_params=pltpu.CompilerParams(collective_id=0, has_side_effects=True, vmem_limit_bytes=67043328),
            cost_estimate=pl.CostEstimate(flops=flops, bytes_accessed=2 ** 26, transcendentals=0),
            name="muon_step",
        )(w_rows, mom_rows, grad_full)

    return jax.shard_map(local_step, mesh=mesh, in_specs=(row_spec, row_spec, grad_spec), out_specs=(row_spec, row_spec), check_vma=False)
```

```python
import functools
import math
import jax
import jax.numpy as jnp
from jax import lax
from jax.experimental import pallas as pl
from jax.experimental.pallas import tpu as pltpu
from jax.sharding import PartitionSpec as P

MOMENTUM_COEF = 0.95
LEARN_RATE = 0.05
WEIGHT_DECAY = 0.2
NORM_EPS = 1e-7
COEF_A = 3.4445
COEF_B = -4.7750
COEF_C = 2.0315
NS_ITERS = 5

CORES = 2
AHEAD = 2
CHUNK = 32
ITERS_PER_STEP = 2
X_PARTS = 4
HOLD = 1
MESH = pl.DeviceIdType.MESH
F32 = jnp.float32
BF16 = jnp.bfloat16


def fused_kernel(group, scale, w_ref, mom_ref, g_ref, fsum, mom_out,
                 mg, fin, own, mout, momin, xin, xbuf0, xbuf1, row, colo0, colo1, poly, ret, nsend, ninbox,
                 s_mg, s_fin, s_fsum, s_own, s_mout, s_mom, s_x, s_n, s_ret,
                 s_gsend, s_xsend, s_nsend, s_rsend, s_momout, s_wload,
                 s_xp, s_xps, s_ap, s_aps, s_keep):
    n_mats, rows, cols = w_ref.shape
    half = rows // 2
    chips = group // CORES
    hr = rows * chips
    me = lax.axis_index("data")
    chip, core = me // CORES, me % CORES
    right, left, far = (chip + 1) % chips, (chip + chips - 1) % chips, (chip + 2) % chips

    def dev(a_chip, a_core):
        return a_chip * CORES + a_core

    mate = dev(chip, 1 - core)

    def owner_chip(m):
        return jnp.where(m < chips, m, 2 * chips - 1 - m)

    def my_mat(e):
        return jnp.where(e == 0, chip, 2 * chips - 1 - chip)

    def grad_rows(m, a_chip, a_core, h):
        start = pl.multiple_of(dev(a_chip, a_core) * rows + h * half, half)
        return g_ref.at[0, m, pl.ds(start, half)]

    def remote(src, dst, send, recv, to):
        return pltpu.make_async_remote_copy(src_ref=src, dst_ref=dst, send_sem=send, recv_sem=recv,
                                            device_id={"data": to}, device_id_type=MESH)

    def wait_bytes(ref, sem, name=None):
        if name is None:
            pltpu.make_async_copy(ref, ref, sem).wait()
        else:
            with jax.named_scope(name):
                pltpu.make_async_copy(ref, ref, sem).wait()

    def issue_raw(m):
        send = s_gsend.at[m]
        for kk in range(CORES):
            remote(grad_rows(m, far, kk, 0), mg.at[m, 0, core], send, s_mg.at[m, 0], dev(right, kk)).start()
            remote(grad_rows(m, far, kk, 1), mg.at[m, 1, core], send, s_mg.at[m, 1], dev(left, kk)).start()
        remote(grad_rows(m, right, 1 - core, 0), mg.at[m, 0, 2], send, s_mg.at[m, 0], mate).start()
        remote(grad_rows(m, left, 1 - core, 1), mg.at[m, 1, 2], send, s_mg.at[m, 1], mate).start()
        for kk in range(CORES):
            remote(grad_rows(m, right, kk, 1), fin.at[m, 1, core], send, s_fin.at[m], dev(right, kk)).start()
            remote(grad_rows(m, left, kk, 0), fin.at[m, 0, core], send, s_fin.at[m], dev(left, kk)).start()
        for h in range(2):
            remote(grad_rows(m, chip, 1 - core, h), fin.at[m, h, 2], send, s_fin.at[m], mate).start()

    def load_own(m):
        slot = m % 3
        pltpu.make_async_copy(grad_rows(m, right, core, 0), own.at[slot, 0], s_own.at[slot]).start()
        pltpu.make_async_copy(grad_rows(m, left, core, 1), own.at[slot, 1], s_own.at[slot]).start()
        for h in range(2):
            pltpu.make_async_copy(grad_rows(m, chip, core, h), own.at[slot, 2 + h], s_own.at[slot]).start()

    def merge_copy(m, h):
        to = dev(right if h == 0 else left, core)
        return remote(mout.at[m % 2, h], fsum.at[m, h], s_mout.at[m % 2, h], s_fsum.at[m, h], to)

    def merge(m):
        slot = m % 3
        wait_bytes(own.at[slot], s_own.at[slot])
        for h in range(2):
            wait_bytes(mg.at[m, h], s_mg.at[m, h], "wait_mg")

            @pl.when(m >= 2)
            def _():
                merge_copy(m - 2, h).wait_send()

            @pl.loop(0, half // min(CHUNK, half))
            def _(i):
                size = min(CHUNK, half)
                at = pl.ds(pl.multiple_of(i * size, size), size)
                total = own[slot, h, at].astype(F32) + mg[m, h, 2, at].astype(F32)
                total = total + (mg[m, h, 0, at].astype(F32) + mg[m, h, 1, at].astype(F32))
                mout[m % 2, h, at] = total
            merge_copy(m, h).start()

    def forward(m, h):
        oc = owner_chip(m)
        late = m // chips
        src = fin.at[m, h, 0]
        dst = xin.at[late, pl.ds(pl.multiple_of(chip * rows + h * half, half), half)]

        @pl.when(oc == chip)
        def _():
            pltpu.make_async_copy(src, dst, s_x.at[late]).start()

        @pl.when(oc != chip)
        def _():
            remote(src, dst, s_xsend.at[m], s_x.at[late], dev(oc, core)).start()

    def finish(m):
        slot = m % 3
        oc = owner_chip(m)
        late = m // chips
        wait_bytes(fin.at[m], s_fin.at[m])
        wait_bytes(momin.at[m % 2], s_mom.at[m % 2])
        size = min(CHUNK, half)
        acc = jnp.zeros((8, 128), F32)
        for h in range(2):
            wait_bytes(fsum.at[m, h], s_fsum.at[m, h], "wait_fsum")

            def part(i, acc):
                at = pl.ds(pl.multiple_of(i * size, size), size)
                mom_at = pl.ds(pl.multiple_of(h * half + i * size, size), size)
                total = own[slot, 2 + h, at].astype(F32) + fin[m, h, 2, at].astype(F32)
                total = total + (fin[m, h, 0, at].astype(F32) + fin[m, h, 1, at].astype(F32))
                total = total + fsum[m, h, at]
                new = MOMENTUM_COEF * momin[m % 2, mom_at] + total
                fsum[m, h, at] = new
                fin[m, h, 0, at] = new.astype(BF16)
                square = new * new
                for r in range(0, size, 8):
                    for q in range(0, cols, 128):
                        acc = acc + square[r:r + 8, q:q + 128]
                return acc

            acc = lax.fori_loop(0, half // size, part, acc)

            @pl.when((late == 0) | (m == n_mats - 1))
            def _():
                forward(m, h)
            pltpu.make_async_copy(fsum.at[m, h], mom_out.at[m, pl.ds(h * half, half)], s_momout.at[m]).start()
        nsend[m] = acc
        sum_to = ninbox.at[late, me]

        @pl.when(oc == chip)
        def _():
            pltpu.make_async_copy(nsend.at[m], sum_to, s_n.at[late]).start()
            remote(nsend.at[m], sum_to, s_nsend.at[m], s_n.at[late], mate).start()

        @pl.when(oc != chip)
        def _():
            for kk in range(CORES):
                remote(nsend.at[m], sum_to, s_nsend.at[m], s_n.at[late], dev(oc, kk)).start()

    def w_load(m):
        wait_bytes(fsum.at[m], s_momout.at[m])
        for h in range(2):
            pltpu.make_async_copy(w_ref.at[m, pl.ds(h * half, half)], fsum.at[m, h], s_wload.at[m]).start()

    first, second = pl.ds(0, hr), pl.ds(hr, hr)

    def to_mate(g, buf, at):
        return remote(buf.at[first, at], buf.at[second, at], s_xps.at[g], s_xp.at[g], mate)

    def ns_begin(e):
        g, buf = e * NS_ITERS, (xbuf0, xbuf1)[(e * NS_ITERS) % 2]
        wait_bytes(xin.at[e], s_x.at[e], "wait_x")
        wait_bytes(ninbox.at[e], s_n.at[e], "wait_n")
        total = jnp.sum(ninbox[e], axis=0)
        total = jnp.sum(jnp.sum(total, axis=0, keepdims=True), axis=1, keepdims=True)
        bound = jnp.sqrt(total) + NORM_EPS

        @pl.loop(0, chips)
        def _(b):
            @pl.loop(0, rows // CHUNK)
            def _(i):
                at = pl.ds(pl.multiple_of(b * rows + i * CHUNK, CHUNK), CHUNK)
                buf[at] = (xin[e, at].astype(F32) / bound).astype(BF16)
            at = pl.ds(pl.multiple_of(b * rows, rows), rows)
            there = pl.ds(pl.multiple_of(hr + b * rows, rows), rows)
            remote(buf.at[at], buf.at[there], s_xps.at[g], s_xp.at[g], mate).start()

    def ns_iter(g, par, last, late):
        cur, nxt, col = ((xbuf0, xbuf1, colo0), (xbuf1, xbuf0, colo1))[par]
        transposed = (((1,), (1,)), ((), ()))
        diag = remote(row.at[:, first], col.at[second], s_aps.at[g], s_ap.at[g], mate)

        with jax.named_scope("gram"):
            prod = lax.dot_general(cur[first], cur[first], transposed, preferred_element_type=F32)
            row[:, first] = prod.astype(BF16)
            diag.start()
        wait_bytes(cur.at[second], s_xp.at[g], "wait_xp")
        wait_bytes(col.at[second], s_ap.at[g], "wait_ap")
        with jax.named_scope("squares"):
            prod = lax.dot_general(cur[first], cur[second], transposed, preferred_element_type=F32)
            prod = prod.astype(BF16)
            row[:, second] = prod
            col[first] = prod
            prod = lax.dot_general(row[...], row[...], transposed, preferred_element_type=F32)
            poly[:, first] = (COEF_B * row[:, first].astype(F32) + COEF_C * prod).astype(BF16)
            prod = jnp.dot(row[...], col[...], preferred_element_type=F32)
            poly[:, second] = (COEF_B * row[:, second].astype(F32) + COEF_C * prod).astype(BF16)
        with jax.named_scope("newx"):
            wide = cols // X_PARTS
            for j in range(X_PARTS):
                at = pl.ds(j * wide, wide)
                prod = jnp.dot(poly[...], cur[:, at], preferred_element_type=F32)
                nxt[first, at] = (COEF_A * cur[first, at].astype(F32) + prod).astype(BF16)
                if not last:
                    to_mate(g + 1, nxt, at).start()
                elif late:
                    give_back(1, nxt, at)
        if last and not late:
            keep = pltpu.make_async_copy(nxt.at[first], xin.at[0], s_keep)
            keep.start()
            keep.wait()
        diag.wait_send()
        wait_bytes(cur.at[first], s_xps.at[g])

    def give_back(e, src, at):
        mat = my_mat(e)
        dst = ret.at[mat, :, at]

        def block(c):
            return src.at[pl.ds(pl.multiple_of(c * rows, rows), rows), at]

        for i in range(1, chips):
            c = (chip + i) % chips
            remote(block(c), dst, s_rsend.at[e], s_ret.at[mat], dev(c, core)).start()
        pltpu.make_async_copy(block(chip), dst, s_ret.at[mat]).start()

    def early_done(s):
        return jnp.clip(ITERS_PER_STEP * (s - chip - 2), 0, NS_ITERS)

    barrier = pltpu.get_barrier_semaphore()
    for i in range(1, group):
        pl.semaphore_signal(barrier, inc=1, device_id={"data": (me + i) % group}, device_id_type=MESH)
    pl.semaphore_wait(barrier, group - 1)

    @pl.loop(0, AHEAD)
    def _(m):
        issue_raw(m)
    load_own(0)

    @pl.loop(0, n_mats + 2)
    def _(s):
        @pl.when(s + AHEAD < n_mats)
        def _():
            issue_raw(s + AHEAD)

        @pl.when(s + 1 < n_mats)
        def _():
            load_own(s + 1)

        @pl.when(s < n_mats)
        def _():
            pltpu.make_async_copy(mom_ref.at[s], momin.at[s % 2], s_mom.at[s % 2]).start()
            merge(s)

        @pl.when(s == n_mats - 1)
        def _():
            @pl.loop(chips, n_mats - 2)
            def _(m):
                for h in range(2):
                    forward(m, h)

        last = s == n_mats + 1
        lo = jnp.where(s >= n_mats, early_done(n_mats - 1), early_done(s - 1))
        hi = jnp.where(last, 2 * NS_ITERS, jnp.where(s >= n_mats, lo, early_done(s)))

        def run(g, carry):
            @pl.when(g == 0)
            def _():
                ns_begin(0)

            @pl.when(g == NS_ITERS)
            def _():
                ns_begin(1)

            @pl.when(g == NS_ITERS + HOLD)
            def _():
                give_back(0, xin.at[0], pl.ds(0, cols))

            end = g % NS_ITERS == NS_ITERS - 1
            for par in range(2):
                @pl.when((g % 2 == par) & jnp.logical_not(end))
                def _():
                    ns_iter(g, par, False, False)
            for e in range(2):
                @pl.when(g == (e + 1) * NS_ITERS - 1)
                def _():
                    ns_iter(g, ((e + 1) * NS_ITERS - 1) % 2, True, e == 1)
            return carry
        lax.fori_loop(lo, hi, run, 0)

        @pl.when((s >= 1) & (s <= n_mats))
        def _():
            finish(s - 1)

        @pl.when(s == n_mats - 1)
        def _():
            for h in range(2):
                forward(n_mats - 2, h)

        @pl.when(s >= 2)
        def _():
            w_load(s - 2)

    @pl.loop(0, n_mats)
    def _(m):
        wait_bytes(ret.at[m], s_ret.at[m], "wait_ret")
        wait_bytes(fsum.at[m], s_wload.at[m])
        size = min(CHUNK, half)
        for h in range(2):
            @pl.loop(0, half // size)
            def _(i):
                at = pl.ds(pl.multiple_of(i * size, size), size)
                ret_at = pl.ds(pl.multiple_of(h * half + i * size, size), size)
                w = fsum[m, h, at]
                fsum[m, h, at] = w - LEARN_RATE * (ret[m, ret_at].astype(F32) * scale + WEIGHT_DECAY * w)

    @pl.loop(0, n_mats)
    def _(m):
        done = g_ref.at[0, m, pl.ds(0, 12 * half)]
        wait_bytes(done, s_gsend.at[m])

        @pl.when(owner_chip(m) == chip)
        def _():
            wait_bytes(nsend.at[0], s_nsend.at[m])

        @pl.when(owner_chip(m) != chip)
        def _():
            wait_bytes(ret.at[m], s_xsend.at[m])
            wait_bytes(nsend.at[pl.ds(0, CORES)], s_nsend.at[m])
    for m in range(n_mats - 2, n_mats):
        for h in range(2):
            merge_copy(m, h).wait_send()
    for e in range(2):
        wait_bytes(xin.at[e, pl.ds(0, (chips - 1) * rows)], s_rsend.at[e])


def solution(mesh):
    group = mesh.shape['data']
    row_spec = P('stage', 'data', None)
    grad_spec = P(('stage', 'data'), None, None, None)

    def local_step(w_rows, mom_rows, grad_full):
        n_mats, rows, cols = w_rows.shape
        half = rows // 2
        n_rows = rows * group
        hr = n_rows // CORES
        scale = 0.2 * math.sqrt(max(n_rows, cols))
        hbm = pl.BlockSpec(memory_space=pl.ANY)
        dma = pltpu.SemaphoreType.DMA
        flops = NS_ITERS * (4 * n_rows * n_rows * cols + 2 * n_rows ** 3)
        w_new, mom_new = pl.pallas_call(
            functools.partial(fused_kernel, group, scale),
            out_shape=(pltpu.VMEM((n_mats, 2, half, cols), F32), jax.ShapeDtypeStruct(w_rows.shape, F32)),
            in_specs=[hbm] * 3,
            out_specs=(pl.BlockSpec(memory_space=pltpu.VMEM), hbm),
            scratch_shapes=[
                pltpu.VMEM((n_mats, 2, 3, half, cols), BF16),
                pltpu.VMEM((n_mats, 2, 3, half, cols), BF16),
                pltpu.VMEM((3, 4, half, cols), BF16),
                pltpu.VMEM((2, 2, half, cols), F32),
                pltpu.VMEM((2, rows, cols), F32),
                pltpu.VMEM((2, hr, cols), BF16),
                pltpu.VMEM((n_rows, cols), BF16),
                pltpu.VMEM((n_rows, cols), BF16),
                pltpu.VMEM((hr, n_rows), BF16),
                pltpu.VMEM((n_rows, hr), BF16),
                pltpu.VMEM((n_rows, hr), BF16),
                pltpu.VMEM((hr, n_rows), BF16),
                pltpu.VMEM((n_mats, rows, cols), BF16),
                pltpu.VMEM((n_mats, 8, 128), F32),
                pltpu.VMEM((2, group, 8, 128), F32),
                dma((n_mats, 2)), dma((n_mats,)), dma((n_mats, 2)), dma((3,)), dma((2, 2)), dma((2,)),
                dma((2,)), dma((2,)), dma((n_mats,)),
                dma((n_mats,)), dma((n_mats,)), dma((n_mats,)), dma((2,)), dma((n_mats,)), dma((n_mats,)),
                dma((2 * NS_ITERS,)), dma((2 * NS_ITERS,)), dma((2 * NS_ITERS,)), dma((2 * NS_ITERS,)), dma,
            ],
            compiler_params=pltpu.CompilerParams(collective_id=0, has_side_effects=True, vmem_limit_bytes=55 * 2 ** 20),
            cost_estimate=pl.CostEstimate(flops=flops, bytes_accessed=2 ** 26, transcendentals=0),
            name="muon_step",
        )(w_rows, mom_rows, grad_full)
        return w_new.reshape(w_rows.shape), mom_new

    return jax.shard_map(local_step, mesh=mesh, in_specs=(row_spec, row_spec, grad_spec), out_specs=(row_spec, row_spec), check_vma=False)
```

```python
import functools
import math
import jax
import jax.numpy as jnp
from jax import lax
from jax.experimental import pallas as pl
from jax.experimental.pallas import tpu as pltpu
from jax.sharding import PartitionSpec as P

MOMENTUM_COEF = 0.95
LEARN_RATE = 0.05
WEIGHT_DECAY = 0.2
NORM_EPS = 1e-7
COEF_A = 3.4445
COEF_B = -4.7750
COEF_C = 2.0315
NS_ITERS = 5

CORES = 2
AHEAD = 2
CHUNK = 32
ITERS_PER_STEP = 2
MG_SLOTS = 4
X_PARTS = 4
HOLD = 1
MESH = pl.DeviceIdType.MESH
F32 = jnp.float32
BF16 = jnp.bfloat16


def fused_kernel(group, scale, w_ref, mom_ref, g_ref, fsum, wbuf,
                 mg, fin, own, mout, momin, xin, xbuf0, xbuf1, row, colo0, colo1, poly, ret, nsend, ninbox,
                 s_mg, s_fin, s_fsum, s_own, s_mout, s_mom, s_x, s_n, s_ret,
                 s_gsend, s_xsend, s_nsend, s_rsend, s_wload, s_free,
                 s_xp, s_xps, s_ap, s_aps, s_keep):
    n_mats, rows, cols = w_ref.shape
    half = rows // 2
    chips = group // CORES
    hr = rows * chips
    me = lax.axis_index("data")
    chip, core = me // CORES, me % CORES
    right, left, far = (chip + 1) % chips, (chip + chips - 1) % chips, (chip + 2) % chips

    def dev(a_chip, a_core):
        return a_chip * CORES + a_core

    mate = dev(chip, 1 - core)

    def owner_chip(m):
        return jnp.where(m < chips, m, 2 * chips - 1 - m)

    def my_mat(e):
        return jnp.where(e == 0, chip, 2 * chips - 1 - chip)

    def grad_rows(m, a_chip, a_core, h):
        start = pl.multiple_of(dev(a_chip, a_core) * rows + h * half, half)
        return g_ref.at[0, m, pl.ds(start, half)]

    def remote(src, dst, send, recv, to):
        return pltpu.make_async_remote_copy(src_ref=src, dst_ref=dst, send_sem=send, recv_sem=recv,
                                            device_id={"data": to}, device_id_type=MESH)

    def wait_bytes(ref, sem, name=None):
        if name is None:
            pltpu.make_async_copy(ref, ref, sem).wait()
        else:
            with jax.named_scope(name):
                pltpu.make_async_copy(ref, ref, sem).wait()

    peers = [dev(left, 0), dev(left, 1), dev(right, 0), dev(right, 1), mate]

    def issue_raw(m):
        send = s_gsend.at[m]

        @pl.when(m >= MG_SLOTS)
        def _():
            pl.semaphore_wait(s_free.at[jnp.maximum(m - MG_SLOTS, 0)], len(peers))
        for kk in range(CORES):
            remote(grad_rows(m, far, kk, 0), mg.at[m % MG_SLOTS, 0, core], send, s_mg.at[m % MG_SLOTS, 0], dev(right, kk)).start()
            remote(grad_rows(m, far, kk, 1), mg.at[m % MG_SLOTS, 1, core], send, s_mg.at[m % MG_SLOTS, 1], dev(left, kk)).start()
        remote(grad_rows(m, right, 1 - core, 0), mg.at[m % MG_SLOTS, 0, 2], send, s_mg.at[m % MG_SLOTS, 0], mate).start()
        remote(grad_rows(m, left, 1 - core, 1), mg.at[m % MG_SLOTS, 1, 2], send, s_mg.at[m % MG_SLOTS, 1], mate).start()
        for kk in range(CORES):
            remote(grad_rows(m, right, kk, 1), fin.at[m, 1, core], send, s_fin.at[m], dev(right, kk)).start()
            remote(grad_rows(m, left, kk, 0), fin.at[m, 0, core], send, s_fin.at[m], dev(left, kk)).start()
        for h in range(2):
            remote(grad_rows(m, chip, 1 - core, h), fin.at[m, h, 2], send, s_fin.at[m], mate).start()

    def load_own(m):
        slot = m % 3
        pltpu.make_async_copy(grad_rows(m, right, core, 0), own.at[slot, 0], s_own.at[slot]).start()
        pltpu.make_async_copy(grad_rows(m, left, core, 1), own.at[slot, 1], s_own.at[slot]).start()
        for h in range(2):
            pltpu.make_async_copy(grad_rows(m, chip, core, h), own.at[slot, 2 + h], s_own.at[slot]).start()

    def merge_copy(m, h):
        to = dev(right if h == 0 else left, core)
        return remote(mout.at[m % 2, h], fsum.at[m, h], s_mout.at[m % 2, h], s_fsum.at[m, h], to)

    def merge(m):
        slot = m % 3
        wait_bytes(own.at[slot], s_own.at[slot])
        for h in range(2):
            wait_bytes(mg.at[m % MG_SLOTS, h], s_mg.at[m % MG_SLOTS, h], "wait_mg")

            @pl.when(m >= 2)
            def _():
                merge_copy(m - 2, h).wait_send()

            @pl.loop(0, half // min(CHUNK, half))
            def _(i):
                size = min(CHUNK, half)
                at = pl.ds(pl.multiple_of(i * size, size), size)
                total = own[slot, h, at].astype(F32) + mg[m % MG_SLOTS, h, 2, at].astype(F32)
                total = total + (mg[m % MG_SLOTS, h, 0, at].astype(F32) + mg[m % MG_SLOTS, h, 1, at].astype(F32))
                mout[m % 2, h, at] = total
            merge_copy(m, h).start()

        @pl.when(m + MG_SLOTS < n_mats)
        def _():
            for peer in peers:
                pl.semaphore_signal(s_free.at[m], inc=1, device_id={"data": peer}, device_id_type=MESH)

    def forward(m, h):
        oc = owner_chip(m)
        late = m // chips
        src = fin.at[m, h, 0]
        dst = xin.at[late, pl.ds(pl.multiple_of(chip * rows + h * half, half), half)]

        @pl.when(oc == chip)
        def _():
            pltpu.make_async_copy(src, dst, s_x.at[late]).start()

        @pl.when(oc != chip)
        def _():
            remote(src, dst, s_xsend.at[m], s_x.at[late], dev(oc, core)).start()

    def finish(m):
        slot = m % 3
        oc = owner_chip(m)
        late = m // chips
        wait_bytes(fin.at[m], s_fin.at[m])
        wait_bytes(momin.at[m % 2], s_mom.at[m % 2])
        size = min(CHUNK, half)
        acc = jnp.zeros((8, 128), F32)
        for h in range(2):
            wait_bytes(fsum.at[m, h], s_fsum.at[m, h], "wait_fsum")

            def part(i, acc):
                at = pl.ds(pl.multiple_of(i * size, size), size)
                mom_at = pl.ds(pl.multiple_of(h * half + i * size, size), size)
                total = own[slot, 2 + h, at].astype(F32) + fin[m, h, 2, at].astype(F32)
                total = total + (fin[m, h, 0, at].astype(F32) + fin[m, h, 1, at].astype(F32))
                total = total + fsum[m, h, at]
                new = MOMENTUM_COEF * momin[m % 2, mom_at] + total
                fsum[m, h, at] = new
                fin[m, h, 0, at] = new.astype(BF16)
                square = new * new
                for r in range(0, size, 8):
                    for q in range(0, cols, 128):
                        acc = acc + square[r:r + 8, q:q + 128]
                return acc

            acc = lax.fori_loop(0, half // size, part, acc)

            @pl.when((late == 0) | (m == n_mats - 1))
            def _():
                forward(m, h)
        nsend[m] = acc
        sum_to = ninbox.at[late, me]

        @pl.when(oc == chip)
        def _():
            pltpu.make_async_copy(nsend.at[m], sum_to, s_n.at[late]).start()
            remote(nsend.at[m], sum_to, s_nsend.at[m], s_n.at[late], mate).start()

        @pl.when(oc != chip)
        def _():
            for kk in range(CORES):
                remote(nsend.at[m], sum_to, s_nsend.at[m], s_n.at[late], dev(oc, kk)).start()

    first, second = pl.ds(0, hr), pl.ds(hr, hr)

    def to_mate(g, buf, at):
        return remote(buf.at[first, at], buf.at[second, at], s_xps.at[g], s_xp.at[g], mate)

    def ns_begin(e):
        g, buf = e * NS_ITERS, (xbuf0, xbuf1)[(e * NS_ITERS) % 2]
        wait_bytes(xin.at[e], s_x.at[e], "wait_x")
        wait_bytes(ninbox.at[e], s_n.at[e], "wait_n")
        total = jnp.sum(ninbox[e], axis=0)
        total = jnp.sum(jnp.sum(total, axis=0, keepdims=True), axis=1, keepdims=True)
        bound = jnp.sqrt(total) + NORM_EPS

        @pl.loop(0, chips)
        def _(b):
            @pl.loop(0, rows // CHUNK)
            def _(i):
                at = pl.ds(pl.multiple_of(b * rows + i * CHUNK, CHUNK), CHUNK)
                buf[at] = (xin[e, at].astype(F32) / bound).astype(BF16)
            at = pl.ds(pl.multiple_of(b * rows, rows), rows)
            there = pl.ds(pl.multiple_of(hr + b * rows, rows), rows)
            remote(buf.at[at], buf.at[there], s_xps.at[g], s_xp.at[g], mate).start()

    def ns_iter(g, par, last, late):
        cur, nxt, col = ((xbuf0, xbuf1, colo0), (xbuf1, xbuf0, colo1))[par]
        transposed = (((1,), (1,)), ((), ()))
        diag = remote(row.at[:, first], col.at[second], s_aps.at[g], s_ap.at[g], mate)

        with jax.named_scope("gram"):
            prod = lax.dot_general(cur[first], cur[first], transposed, preferred_element_type=F32)
            row[:, first] = prod.astype(BF16)
            diag.start()
        wait_bytes(cur.at[second], s_xp.at[g], "wait_xp")
        with jax.named_scope("squares"):
            prod = lax.dot_general(cur[first], cur[second], transposed, preferred_element_type=F32)
            prod = prod.astype(BF16)
            row[:, second] = prod
            col[first] = prod
            prod = lax.dot_general(row[...], row[...], transposed, preferred_element_type=F32)
            poly[:, first] = (COEF_B * row[:, first].astype(F32) + COEF_C * prod).astype(BF16)
        wait_bytes(col.at[second], s_ap.at[g], "wait_ap")
        with jax.named_scope("newx"):
            prod = jnp.dot(row[...], col[...], preferred_element_type=F32)
            poly[:, second] = (COEF_B * row[:, second].astype(F32) + COEF_C * prod).astype(BF16)
            wide = cols // X_PARTS
            for j in range(X_PARTS):
                at = pl.ds(j * wide, wide)
                prod = jnp.dot(poly[...], cur[:, at], preferred_element_type=F32)
                nxt[first, at] = (COEF_A * cur[first, at].astype(F32) + prod).astype(BF16)
                if not last:
                    to_mate(g + 1, nxt, at).start()
                elif late:
                    give_back(1, nxt, at)
        if last and not late:
            keep = pltpu.make_async_copy(nxt.at[first], xin.at[0], s_keep)
            keep.start()
            keep.wait()
        diag.wait_send()
        wait_bytes(cur.at[first], s_xps.at[g])

    def give_back(e, src, at):
        mat = my_mat(e)
        dst = ret.at[mat, :, at]

        def block(c):
            return src.at[pl.ds(pl.multiple_of(c * rows, rows), rows), at]

        for i in range(1, chips):
            c = (chip + i) % chips
            remote(block(c), dst, s_rsend.at[e], s_ret.at[mat], dev(c, core)).start()
        pltpu.make_async_copy(block(chip), dst, s_ret.at[mat]).start()

    def early_done(s):
        return jnp.clip(ITERS_PER_STEP * (s - chip - 2), 0, NS_ITERS)

    barrier = pltpu.get_barrier_semaphore()
    for i in range(1, group):
        pl.semaphore_signal(barrier, inc=1, device_id={"data": (me + i) % group}, device_id_type=MESH)
    pl.semaphore_wait(barrier, group - 1)

    @pl.loop(0, AHEAD)
    def _(m):
        issue_raw(m)
    load_own(0)
    pltpu.make_async_copy(w_ref, wbuf, s_wload).start()

    @pl.loop(0, n_mats + 2)
    def _(s):
        @pl.when(s + AHEAD < n_mats)
        def _():
            issue_raw(s + AHEAD)

        @pl.when(s + 1 < n_mats)
        def _():
            load_own(s + 1)

        @pl.when(s < n_mats)
        def _():
            pltpu.make_async_copy(mom_ref.at[s], momin.at[s % 2], s_mom.at[s % 2]).start()
            merge(s)

        @pl.when(s == n_mats - 1)
        def _():
            @pl.loop(chips, n_mats - 2)
            def _(m):
                for h in range(2):
                    forward(m, h)

        last = s == n_mats + 1
        lo = jnp.where(s >= n_mats, early_done(n_mats - 1), early_done(s - 1))
        hi = jnp.where(last, 2 * NS_ITERS, jnp.where(s >= n_mats, lo, early_done(s)))

        def run(g, carry):
            @pl.when(g == 0)
            def _():
                ns_begin(0)

            @pl.when(g == NS_ITERS)
            def _():
                ns_begin(1)

            @pl.when(g == NS_ITERS + HOLD)
            def _():
                give_back(0, xin.at[0], pl.ds(0, cols))

            end = g % NS_ITERS == NS_ITERS - 1
            for par in range(2):
                @pl.when((g % 2 == par) & jnp.logical_not(end))
                def _():
                    ns_iter(g, par, False, False)
            for e in range(2):
                @pl.when(g == (e + 1) * NS_ITERS - 1)
                def _():
                    ns_iter(g, ((e + 1) * NS_ITERS - 1) % 2, True, e == 1)
            return carry
        lax.fori_loop(lo, hi, run, 0)

        @pl.when((s >= 1) & (s <= n_mats))
        def _():
            finish(s - 1)

        @pl.when(s == n_mats - 1)
        def _():
            for h in range(2):
                forward(n_mats - 2, h)

    wait_bytes(wbuf, s_wload)

    @pl.loop(0, n_mats)
    def _(m):
        wait_bytes(ret.at[m], s_ret.at[m], "wait_ret")
        @pl.loop(0, rows // CHUNK)
        def _(i):
            at = pl.ds(pl.multiple_of(i * CHUNK, CHUNK), CHUNK)
            w = wbuf[m, at]
            wbuf[m, at] = w - LEARN_RATE * (ret[m, at].astype(F32) * scale + WEIGHT_DECAY * w)

    @pl.loop(0, n_mats)
    def _(m):
        done = g_ref.at[0, m, pl.ds(0, 12 * half)]
        wait_bytes(done, s_gsend.at[m])

        @pl.when(owner_chip(m) == chip)
        def _():
            wait_bytes(nsend.at[0], s_nsend.at[m])

        @pl.when(owner_chip(m) != chip)
        def _():
            wait_bytes(ret.at[m], s_xsend.at[m])
            wait_bytes(nsend.at[pl.ds(0, CORES)], s_nsend.at[m])
    for m in range(n_mats - 2, n_mats):
        for h in range(2):
            merge_copy(m, h).wait_send()
    for e in range(2):
        wait_bytes(xin.at[e, pl.ds(0, (chips - 1) * rows)], s_rsend.at[e])


def flush_kernel(parts, w_ref, mom_ref, w_out, mom_out, sem):
    step = w_ref.shape[0] // parts
    copies = []
    for p in range(parts):
        at = pl.ds(p * step, step)
        copies.append(pltpu.make_async_copy(w_ref.at[at], w_out.at[at], sem.at[0, p]))
        copies.append(pltpu.make_async_copy(mom_ref.at[at], mom_out.at[at], sem.at[1, p]))
    for copy in copies:
        copy.start()
    for copy in copies:
        copy.wait()


def solution(mesh):
    group = mesh.shape['data']
    row_spec = P('stage', 'data', None)
    grad_spec = P(('stage', 'data'), None, None, None)

    def local_step(w_rows, mom_rows, grad_full):
        n_mats, rows, cols = w_rows.shape
        half = rows // 2
        n_rows = rows * group
        hr = n_rows // CORES
        scale = 0.2 * math.sqrt(max(n_rows, cols))
        hbm = pl.BlockSpec(memory_space=pl.ANY)
        dma = pltpu.SemaphoreType.DMA
        flops = NS_ITERS * (4 * n_rows * n_rows * cols + 2 * n_rows ** 3)
        mom_new, w_new = pl.pallas_call(
            functools.partial(fused_kernel, group, scale),
            out_shape=(pltpu.VMEM((n_mats, 2, half, cols), F32), pltpu.VMEM(w_rows.shape, F32)),
            in_specs=[hbm] * 3,
            out_specs=(pl.BlockSpec(memory_space=pltpu.VMEM), pl.BlockSpec(memory_space=pltpu.VMEM)),
            scratch_shapes=[
                pltpu.VMEM((MG_SLOTS, 2, 3, half, cols), BF16),
                pltpu.VMEM((n_mats, 2, 3, half, cols), BF16),
                pltpu.VMEM((3, 4, half, cols), BF16),
                pltpu.VMEM((2, 2, half, cols), F32),
                pltpu.VMEM((2, rows, cols), F32),
                pltpu.VMEM((2, hr, cols), BF16),
                pltpu.VMEM((n_rows, cols), BF16),
                pltpu.VMEM((n_rows, cols), BF16),
                pltpu.VMEM((hr, n_rows), BF16),
                pltpu.VMEM((n_rows, hr), BF16),
                pltpu.VMEM((n_rows, hr), BF16),
                pltpu.VMEM((hr, n_rows), BF16),
                pltpu.VMEM((n_mats, rows, cols), BF16),
                pltpu.VMEM((n_mats, 8, 128), F32),
                pltpu.VMEM((2, group, 8, 128), F32),
                dma((n_mats, 2)), dma((n_mats,)), dma((n_mats, 2)), dma((3,)), dma((2, 2)), dma((2,)),
                dma((2,)), dma((2,)), dma((n_mats,)),
                dma((n_mats,)), dma((n_mats,)), dma((n_mats,)), dma((2,)), dma, pltpu.SemaphoreType.REGULAR((n_mats,)),
                dma((2 * NS_ITERS,)), dma((2 * NS_ITERS,)), dma((2 * NS_ITERS,)), dma((2 * NS_ITERS,)), dma,
            ],
            compiler_params=pltpu.CompilerParams(collective_id=0, has_side_effects=True, vmem_limit_bytes=47 * 2 ** 20),
            cost_estimate=pl.CostEstimate(flops=flops, bytes_accessed=2 ** 26, transcendentals=0),
            name="muon_step",
        )(w_rows, mom_rows, grad_full)
        mom_new = mom_new.reshape(w_rows.shape)
        parts = 4
        return pl.pallas_call(
            functools.partial(flush_kernel, parts),
            out_shape=(jax.ShapeDtypeStruct(w_rows.shape, F32), jax.ShapeDtypeStruct(w_rows.shape, F32)),
            in_specs=[pl.BlockSpec(memory_space=pltpu.VMEM)] * 2,
            out_specs=(hbm, hbm),
            scratch_shapes=[dma((2, parts))],
            compiler_params=pltpu.CompilerParams(vmem_limit_bytes=2 ** 20),
            cost_estimate=pl.CostEstimate(flops=0, bytes_accessed=2 * w_rows.size * 4, transcendentals=0),
            name="flush",
        )(w_new, mom_new)

    return jax.shard_map(local_step, mesh=mesh, in_specs=(row_spec, row_spec, grad_spec), out_specs=(row_spec, row_spec), check_vma=False)
```

```python
import functools
import math
import jax
import jax.numpy as jnp
from jax import lax
from jax.experimental import pallas as pl
from jax.experimental.pallas import tpu as pltpu
from jax.sharding import PartitionSpec as P

MOMENTUM_COEF = 0.95
LEARN_RATE = 0.05
WEIGHT_DECAY = 0.2
NORM_EPS = 1e-7
COEF_A = 3.4445
COEF_B = -4.7750
COEF_C = 2.0315
NS_ITERS = 5

CORES = 2
AHEAD = 2
CHUNK = 32
ITERS_PER_STEP = 2
MG_SLOTS = 4
X_PARTS = 4
HOLD = 0
MESH = pl.DeviceIdType.MESH
F32 = jnp.float32
BF16 = jnp.bfloat16


def fused_kernel(group, scale, w_ref, mom_ref, g_ref, fsum, wbuf,
                 mg, fin, own, mout, momin, xin, xbuf0, xbuf1, row, colo0, colo1, poly, ret, nsend, ninbox,
                 s_mg, s_fin, s_fsum, s_own, s_mout, s_mom, s_x, s_n, s_ret,
                 s_gsend, s_xsend, s_nsend, s_rsend, s_wload, s_free,
                 s_xp, s_xps, s_ap, s_aps, s_keep):
    n_mats, rows, cols = w_ref.shape
    half = rows // 2
    chips = group // CORES
    hr = rows * chips
    me = lax.axis_index("data")
    chip, core = me // CORES, me % CORES
    right, left, far = (chip + 1) % chips, (chip + chips - 1) % chips, (chip + 2) % chips

    def dev(a_chip, a_core):
        return a_chip * CORES + a_core

    mate = dev(chip, 1 - core)

    def owner_chip(m):
        return jnp.where(m < chips, m, 2 * chips - 1 - m)

    def my_mat(e):
        return jnp.where(e == 0, chip, 2 * chips - 1 - chip)

    def grad_rows(m, a_chip, a_core, h):
        start = pl.multiple_of(dev(a_chip, a_core) * rows + h * half, half)
        return g_ref.at[0, m, pl.ds(start, half)]

    def remote(src, dst, send, recv, to):
        return pltpu.make_async_remote_copy(src_ref=src, dst_ref=dst, send_sem=send, recv_sem=recv,
                                            device_id={"data": to}, device_id_type=MESH)

    def wait_bytes(ref, sem, name=None):
        if name is None:
            pltpu.make_async_copy(ref, ref, sem).wait()
        else:
            with jax.named_scope(name):
                pltpu.make_async_copy(ref, ref, sem).wait()

    peers = [dev(left, 0), dev(left, 1), dev(right, 0), dev(right, 1), mate]

    def issue_raw(m):
        send = s_gsend.at[m]

        @pl.when(m >= MG_SLOTS)
        def _():
            pl.semaphore_wait(s_free.at[jnp.maximum(m - MG_SLOTS, 0)], len(peers))
        for kk in range(CORES):
            remote(grad_rows(m, far, kk, 0), mg.at[m % MG_SLOTS, 0, core], send, s_mg.at[m % MG_SLOTS, 0], dev(right, kk)).start()
            remote(grad_rows(m, far, kk, 1), mg.at[m % MG_SLOTS, 1, core], send, s_mg.at[m % MG_SLOTS, 1], dev(left, kk)).start()
        remote(grad_rows(m, right, 1 - core, 0), mg.at[m % MG_SLOTS, 0, 2], send, s_mg.at[m % MG_SLOTS, 0], mate).start()
        remote(grad_rows(m, left, 1 - core, 1), mg.at[m % MG_SLOTS, 1, 2], send, s_mg.at[m % MG_SLOTS, 1], mate).start()
        for kk in range(CORES):
            remote(grad_rows(m, right, kk, 1), fin.at[m, 1, core], send, s_fin.at[m], dev(right, kk)).start()
            remote(grad_rows(m, left, kk, 0), fin.at[m, 0, core], send, s_fin.at[m], dev(left, kk)).start()
        for h in range(2):
            remote(grad_rows(m, chip, 1 - core, h), fin.at[m, h, 2], send, s_fin.at[m], mate).start()

    def load_own(m):
        slot = m % 3
        pltpu.make_async_copy(grad_rows(m, right, core, 0), own.at[slot, 0], s_own.at[slot]).start()
        pltpu.make_async_copy(grad_rows(m, left, core, 1), own.at[slot, 1], s_own.at[slot]).start()
        for h in range(2):
            pltpu.make_async_copy(grad_rows(m, chip, core, h), own.at[slot, 2 + h], s_own.at[slot]).start()

    def merge_copy(m, h):
        to = dev(right if h == 0 else left, core)
        return remote(mout.at[m % 2, h], fsum.at[m, h], s_mout.at[m % 2, h], s_fsum.at[m, h], to)

    def merge(m):
        slot = m % 3
        wait_bytes(own.at[slot], s_own.at[slot])
        for h in range(2):
            wait_bytes(mg.at[m % MG_SLOTS, h], s_mg.at[m % MG_SLOTS, h], "wait_mg")

            @pl.when(m >= 2)
            def _():
                merge_copy(m - 2, h).wait_send()

            @pl.loop(0, half // min(CHUNK, half))
            def _(i):
                size = min(CHUNK, half)
                at = pl.ds(pl.multiple_of(i * size, size), size)
                total = own[slot, h, at].astype(F32) + mg[m % MG_SLOTS, h, 2, at].astype(F32)
                total = total + (mg[m % MG_SLOTS, h, 0, at].astype(F32) + mg[m % MG_SLOTS, h, 1, at].astype(F32))
                mout[m % 2, h, at] = total
            merge_copy(m, h).start()

        @pl.when(m + MG_SLOTS < n_mats)
        def _():
            for peer in peers:
                pl.semaphore_signal(s_free.at[m], inc=1, device_id={"data": peer}, device_id_type=MESH)

    def forward(m, h, near=True, distant=True):
        oc = owner_chip(m)
        late = m // chips
        wanted = oc != chip
        if not near:
            wanted = oc == far
        if not distant:
            wanted = wanted & (oc != far)
        src = fin.at[m, h, 0]
        dst = xin.at[late, pl.ds(pl.multiple_of(chip * rows + h * half, half), half)]

        if near:
            @pl.when(oc == chip)
            def _():
                pltpu.make_async_copy(src, dst, s_x.at[late, chip]).start()

        @pl.when(wanted)
        def _():
            remote(src, dst, s_xsend.at[m], s_x.at[late, chip], dev(oc, core)).start()

    def finish(m):
        slot = m % 3
        oc = owner_chip(m)
        late = m // chips
        wait_bytes(fin.at[m], s_fin.at[m])
        wait_bytes(momin.at[m % 2], s_mom.at[m % 2])
        size = min(CHUNK, half)
        acc = jnp.zeros((8, 128), F32)
        for h in range(2):
            wait_bytes(fsum.at[m, h], s_fsum.at[m, h], "wait_fsum")

            def part(i, acc):
                at = pl.ds(pl.multiple_of(i * size, size), size)
                mom_at = pl.ds(pl.multiple_of(h * half + i * size, size), size)
                total = own[slot, 2 + h, at].astype(F32) + fin[m, h, 2, at].astype(F32)
                total = total + (fin[m, h, 0, at].astype(F32) + fin[m, h, 1, at].astype(F32))
                total = total + fsum[m, h, at]
                new = MOMENTUM_COEF * momin[m % 2, mom_at] + total
                fsum[m, h, at] = new
                fin[m, h, 0, at] = new.astype(BF16)
                square = new * new
                for r in range(0, size, 8):
                    for q in range(0, cols, 128):
                        acc = acc + square[r:r + 8, q:q + 128]
                return acc

            acc = lax.fori_loop(0, half // size, part, acc)
            if h == 1:
                nsend[m] = acc
                sum_to = ninbox.at[late, me]

                @pl.when(oc == chip)
                def _():
                    pltpu.make_async_copy(nsend.at[m], sum_to, s_n.at[late]).start()
                    remote(nsend.at[m], sum_to, s_nsend.at[m], s_n.at[late], mate).start()

                @pl.when(oc != chip)
                def _():
                    for kk in range(CORES):
                        remote(nsend.at[m], sum_to, s_nsend.at[m], s_n.at[late], dev(oc, kk)).start()

            @pl.when((late == 0) | (m == n_mats - 1))
            def _():
                forward(m, h)

    first, second = pl.ds(0, hr), pl.ds(hr, hr)

    def to_mate(g, buf, at):
        return remote(buf.at[first, at], buf.at[second, at], s_xps.at[g], s_xp.at[g], mate)

    def ns_begin(e):
        g, buf = e * NS_ITERS, (xbuf0, xbuf1)[(e * NS_ITERS) % 2]
        wait_bytes(ninbox.at[e], s_n.at[e], "wait_n")
        total = jnp.sum(ninbox[e], axis=0)
        total = jnp.sum(jnp.sum(total, axis=0, keepdims=True), axis=1, keepdims=True)
        bound = jnp.sqrt(total) + NORM_EPS

        @pl.loop(0, chips)
        def _(step):
            away = jnp.where(step == 2, 3, jnp.where(step == 3, 2, step))
            b = (chip + away) % chips
            here = pl.ds(pl.multiple_of(b * rows, rows), rows)
            wait_bytes(xin.at[e, here], s_x.at[e, b], "wait_x")

            @pl.loop(0, rows // CHUNK)
            def _(i):
                at = pl.ds(pl.multiple_of(b * rows + i * CHUNK, CHUNK), CHUNK)
                buf[at] = (xin[e, at].astype(F32) / bound).astype(BF16)
            there = pl.ds(pl.multiple_of(hr + b * rows, rows), rows)
            remote(buf.at[here], buf.at[there], s_xps.at[g], s_xp.at[g], mate).start()

    def ns_iter(g, par, last, late):
        cur, nxt, col = ((xbuf0, xbuf1, colo0), (xbuf1, xbuf0, colo1))[par]
        transposed = (((1,), (1,)), ((), ()))
        diag = remote(row.at[:, first], col.at[second], s_aps.at[g], s_ap.at[g], mate)

        with jax.named_scope("gram"):
            prod = lax.dot_general(cur[first], cur[first], transposed, preferred_element_type=F32)
            row[:, first] = prod.astype(BF16)
            diag.start()
        wait_bytes(cur.at[second], s_xp.at[g], "wait_xp")
        with jax.named_scope("squares"):
            prod = lax.dot_general(cur[first], cur[second], transposed, preferred_element_type=F32)
            prod = prod.astype(BF16)
            row[:, second] = prod
            col[first] = prod
            prod = lax.dot_general(row[...], row[...], transposed, preferred_element_type=F32)
            poly[:, first] = (COEF_B * row[:, first].astype(F32) + COEF_C * prod).astype(BF16)
        wait_bytes(col.at[second], s_ap.at[g], "wait_ap")
        with jax.named_scope("newx"):
            prod = jnp.dot(row[...], col[...], preferred_element_type=F32)
            poly[:, second] = (COEF_B * row[:, second].astype(F32) + COEF_C * prod).astype(BF16)
            wide = cols // X_PARTS
            for j in range(X_PARTS):
                at = pl.ds(j * wide, wide)
                prod = jnp.dot(poly[...], cur[:, at], preferred_element_type=F32)
                nxt[first, at] = (COEF_A * cur[first, at].astype(F32) + prod).astype(BF16)
                if not last:
                    to_mate(g + 1, nxt, at).start()
                elif late:
                    give_back(1, nxt, at)
        if last and not late:
            keep = pltpu.make_async_copy(nxt.at[first], xin.at[0], s_keep)
            keep.start()
            keep.wait()
        diag.wait_send()
        wait_bytes(cur.at[first], s_xps.at[g])

    def give_back(e, src, at):
        mat = my_mat(e)
        dst = ret.at[mat, :, at]

        def block(c):
            return src.at[pl.ds(pl.multiple_of(c * rows, rows), rows), at]

        for i in range(1, chips):
            c = (chip + i) % chips
            remote(block(c), dst, s_rsend.at[e], s_ret.at[mat], dev(c, core)).start()
        pltpu.make_async_copy(block(chip), dst, s_ret.at[mat]).start()

    def early_done(s):
        return jnp.clip(ITERS_PER_STEP * (s - chip - 2), 0, NS_ITERS)

    barrier = pltpu.get_barrier_semaphore()
    for i in range(1, group):
        pl.semaphore_signal(barrier, inc=1, device_id={"data": (me + i) % group}, device_id_type=MESH)
    pl.semaphore_wait(barrier, group - 1)

    @pl.loop(0, AHEAD)
    def _(m):
        issue_raw(m)
    load_own(0)
    pltpu.make_async_copy(w_ref, wbuf, s_wload).start()

    @pl.loop(0, n_mats + 2)
    def _(s):
        @pl.when(s + AHEAD < n_mats)
        def _():
            issue_raw(s + AHEAD)

        @pl.when(s + 1 < n_mats)
        def _():
            load_own(s + 1)

        @pl.when(s < n_mats)
        def _():
            pltpu.make_async_copy(mom_ref.at[s], momin.at[s % 2], s_mom.at[s % 2]).start()
            merge(s)

        last = s == n_mats + 1
        lo = jnp.where(s >= n_mats, early_done(n_mats - 1), early_done(s - 1))
        hi = jnp.where(last, 2 * NS_ITERS, jnp.where(s >= n_mats, lo, early_done(s)))

        def run(g, carry):
            @pl.when(g == 0)
            def _():
                ns_begin(0)

            @pl.when(g == NS_ITERS)
            def _():
                ns_begin(1)

            @pl.when(g == NS_ITERS + HOLD)
            def _():
                give_back(0, xin.at[0], pl.ds(0, cols))

            end = g % NS_ITERS == NS_ITERS - 1
            for par in range(2):
                @pl.when((g % 2 == par) & jnp.logical_not(end))
                def _():
                    ns_iter(g, par, False, False)
            for e in range(2):
                @pl.when(g == (e + 1) * NS_ITERS - 1)
                def _():
                    ns_iter(g, ((e + 1) * NS_ITERS - 1) % 2, True, e == 1)
            return carry
        lax.fori_loop(lo, hi, run, 0)

        @pl.when((s >= 1) & (s <= n_mats))
        def _():
            finish(s - 1)

        for when, near in ((n_mats - 1, True), (n_mats, False)):
            @pl.when(s == when)
            def _():
                @pl.loop(chips, n_mats - 1)
                def _(m):
                    for h in range(2):
                        forward(m, h, near=near, distant=not near)

    wait_bytes(wbuf, s_wload)

    @pl.loop(0, n_mats)
    def _(m):
        wait_bytes(ret.at[m], s_ret.at[m], "wait_ret")
        @pl.loop(0, rows // CHUNK)
        def _(i):
            at = pl.ds(pl.multiple_of(i * CHUNK, CHUNK), CHUNK)
            w = wbuf[m, at]
            wbuf[m, at] = w - LEARN_RATE * (ret[m, at].astype(F32) * scale + WEIGHT_DECAY * w)

    @pl.loop(0, n_mats)
    def _(m):
        done = g_ref.at[0, m, pl.ds(0, 12 * half)]
        wait_bytes(done, s_gsend.at[m])

        @pl.when(owner_chip(m) == chip)
        def _():
            wait_bytes(nsend.at[0], s_nsend.at[m])

        @pl.when(owner_chip(m) != chip)
        def _():
            wait_bytes(ret.at[m], s_xsend.at[m])
            wait_bytes(nsend.at[pl.ds(0, CORES)], s_nsend.at[m])
    for m in range(n_mats - 2, n_mats):
        for h in range(2):
            merge_copy(m, h).wait_send()
    for e in range(2):
        wait_bytes(xin.at[e, pl.ds(0, (chips - 1) * rows)], s_rsend.at[e])


def flush_kernel(parts, w_ref, mom_ref, w_out, mom_out, sem):
    step = w_ref.shape[0] // parts
    copies = []
    for p in range(parts):
        at = pl.ds(p * step, step)
        copies.append(pltpu.make_async_copy(w_ref.at[at], w_out.at[at], sem.at[0, p]))
        copies.append(pltpu.make_async_copy(mom_ref.at[at], mom_out.at[at], sem.at[1, p]))
    for copy in copies:
        copy.start()
    for copy in copies:
        copy.wait()


def solution(mesh):
    group = mesh.shape['data']
    row_spec = P('stage', 'data', None)
    grad_spec = P(('stage', 'data'), None, None, None)

    def local_step(w_rows, mom_rows, grad_full):
        n_mats, rows, cols = w_rows.shape
        half = rows // 2
        n_rows = rows * group
        chips = group // CORES
        hr = n_rows // CORES
        scale = 0.2 * math.sqrt(max(n_rows, cols))
        hbm = pl.BlockSpec(memory_space=pl.ANY)
        dma = pltpu.SemaphoreType.DMA
        flops = NS_ITERS * (4 * n_rows * n_rows * cols + 2 * n_rows ** 3)
        mom_new, w_new = pl.pallas_call(
            functools.partial(fused_kernel, group, scale),
            out_shape=(pltpu.VMEM((n_mats, 2, half, cols), F32), pltpu.VMEM(w_rows.shape, F32)),
            in_specs=[hbm] * 3,
            out_specs=(pl.BlockSpec(memory_space=pltpu.VMEM), pl.BlockSpec(memory_space=pltpu.VMEM)),
            scratch_shapes=[
                pltpu.VMEM((MG_SLOTS, 2, 3, half, cols), BF16),
                pltpu.VMEM((n_mats, 2, 3, half, cols), BF16),
                pltpu.VMEM((3, 4, half, cols), BF16),
                pltpu.VMEM((2, 2, half, cols), F32),
                pltpu.VMEM((2, rows, cols), F32),
                pltpu.VMEM((2, hr, cols), BF16),
                pltpu.VMEM((n_rows, cols), BF16),
                pltpu.VMEM((n_rows, cols), BF16),
                pltpu.VMEM((hr, n_rows), BF16),
                pltpu.VMEM((n_rows, hr), BF16),
                pltpu.VMEM((n_rows, hr), BF16),
                pltpu.VMEM((hr, n_rows), BF16),
                pltpu.VMEM((n_mats, rows, cols), BF16),
                pltpu.VMEM((n_mats, 8, 128), F32),
                pltpu.VMEM((2, group, 8, 128), F32),
                dma((n_mats, 2)), dma((n_mats,)), dma((n_mats, 2)), dma((3,)), dma((2, 2)), dma((2,)),
                dma((2, chips)), dma((2,)), dma((n_mats,)),
                dma((n_mats,)), dma((n_mats,)), dma((n_mats,)), dma((2,)), dma, pltpu.SemaphoreType.REGULAR((n_mats,)),
                dma((2 * NS_ITERS,)), dma((2 * NS_ITERS,)), dma((2 * NS_ITERS,)), dma((2 * NS_ITERS,)), dma,
            ],
            compiler_params=pltpu.CompilerParams(collective_id=0, has_side_effects=True, vmem_limit_bytes=47 * 2 ** 20),
            cost_estimate=pl.CostEstimate(flops=flops, bytes_accessed=2 ** 26, transcendentals=0),
            name="muon_step",
        )(w_rows, mom_rows, grad_full)
        mom_new = mom_new.reshape(w_rows.shape)
        parts = 4
        return pl.pallas_call(
            functools.partial(flush_kernel, parts),
            out_shape=(jax.ShapeDtypeStruct(w_rows.shape, F32), jax.ShapeDtypeStruct(w_rows.shape, F32)),
            in_specs=[pl.BlockSpec(memory_space=pltpu.VMEM)] * 2,
            out_specs=(hbm, hbm),
            scratch_shapes=[dma((2, parts))],
            compiler_params=pltpu.CompilerParams(vmem_limit_bytes=2 ** 20),
            cost_estimate=pl.CostEstimate(flops=0, bytes_accessed=2 * w_rows.size * 4, transcendentals=0),
            name="flush",
        )(w_new, mom_new)

    return jax.shard_map(local_step, mesh=mesh, in_specs=(row_spec, row_spec, grad_spec), out_specs=(row_spec, row_spec), check_vma=False)
```

```python
import functools
import math
import jax
import jax.numpy as jnp
from jax import lax
from jax.experimental import pallas as pl
from jax.experimental.pallas import tpu as pltpu
from jax.sharding import PartitionSpec as P

MOMENTUM_COEF = 0.95
LEARN_RATE = 0.05
WEIGHT_DECAY = 0.2
NORM_EPS = 1e-7
COEF_A = 3.4445
COEF_B = -4.7750
COEF_C = 2.0315
NS_ITERS = 5

CORES = 2
AHEAD = 2
CHUNK = 32
ITERS_PER_STEP = 2
MG_SLOTS = 4
X_PARTS = 4
HOLD = 1
MESH = pl.DeviceIdType.MESH
F32 = jnp.float32
BF16 = jnp.bfloat16


def fused_kernel(group, w_ref, mom_ref, g_ref, fsum, wbuf, ret,
                 mg, fin, own, mout, momin, xin, xbuf0, xbuf1, row, colo0, colo1, poly, nsend, ninbox,
                 s_mg, s_fin, s_fsum, s_own, s_mout, s_mom, s_x, s_n, s_ret,
                 s_gsend, s_xsend, s_nsend, s_rsend, s_wload, s_free,
                 s_xp, s_xps, s_ap, s_aps, s_keep):
    n_mats, rows, cols = w_ref.shape
    half = rows // 2
    chips = group // CORES
    hr = rows * chips
    me = lax.axis_index("data")
    chip, core = me // CORES, me % CORES
    right, left, far = (chip + 1) % chips, (chip + chips - 1) % chips, (chip + 2) % chips

    def dev(a_chip, a_core):
        return a_chip * CORES + a_core

    mate = dev(chip, 1 - core)

    def owner_chip(m):
        return jnp.where(m < chips, m, 2 * chips - 1 - m)

    def my_mat(e):
        return jnp.where(e == 0, chip, 2 * chips - 1 - chip)

    def grad_rows(m, a_chip, a_core, h):
        start = pl.multiple_of(dev(a_chip, a_core) * rows + h * half, half)
        return g_ref.at[0, m, pl.ds(start, half)]

    def remote(src, dst, send, recv, to):
        return pltpu.make_async_remote_copy(src_ref=src, dst_ref=dst, send_sem=send, recv_sem=recv,
                                            device_id={"data": to}, device_id_type=MESH)

    def wait_bytes(ref, sem, name=None):
        if name is None:
            pltpu.make_async_copy(ref, ref, sem).wait()
        else:
            with jax.named_scope(name):
                pltpu.make_async_copy(ref, ref, sem).wait()

    peers = [dev(left, 0), dev(left, 1), dev(right, 0), dev(right, 1), mate]

    def issue_raw(m):
        send = s_gsend.at[m]

        @pl.when(m >= MG_SLOTS)
        def _():
            pl.semaphore_wait(s_free.at[jnp.maximum(m - MG_SLOTS, 0)], len(peers))
        for kk in range(CORES):
            remote(grad_rows(m, far, kk, 0), mg.at[m % MG_SLOTS, 0, core], send, s_mg.at[m % MG_SLOTS, 0], dev(right, kk)).start()
            remote(grad_rows(m, far, kk, 1), mg.at[m % MG_SLOTS, 1, core], send, s_mg.at[m % MG_SLOTS, 1], dev(left, kk)).start()
        remote(grad_rows(m, right, 1 - core, 0), mg.at[m % MG_SLOTS, 0, 2], send, s_mg.at[m % MG_SLOTS, 0], mate).start()
        remote(grad_rows(m, left, 1 - core, 1), mg.at[m % MG_SLOTS, 1, 2], send, s_mg.at[m % MG_SLOTS, 1], mate).start()
        for kk in range(CORES):
            remote(grad_rows(m, right, kk, 1), fin.at[m, 1, core], send, s_fin.at[m], dev(right, kk)).start()
            remote(grad_rows(m, left, kk, 0), fin.at[m, 0, core], send, s_fin.at[m], dev(left, kk)).start()
        for h in range(2):
            remote(grad_rows(m, chip, 1 - core, h), fin.at[m, h, 2], send, s_fin.at[m], mate).start()

    def load_own(m):
        slot = m % 3
        pltpu.make_async_copy(grad_rows(m, right, core, 0), own.at[slot, 0], s_own.at[slot]).start()
        pltpu.make_async_copy(grad_rows(m, left, core, 1), own.at[slot, 1], s_own.at[slot]).start()
        for h in range(2):
            pltpu.make_async_copy(grad_rows(m, chip, core, h), own.at[slot, 2 + h], s_own.at[slot]).start()

    def merge_copy(m, h):
        to = dev(right if h == 0 else left, core)
        return remote(mout.at[m % 2, h], fsum.at[m, h], s_mout.at[m % 2, h], s_fsum.at[m, h], to)

    def merge(m):
        slot = m % 3
        wait_bytes(own.at[slot], s_own.at[slot])
        for h in range(2):
            wait_bytes(mg.at[m % MG_SLOTS, h], s_mg.at[m % MG_SLOTS, h], "wait_mg")

            @pl.when(m >= 2)
            def _():
                merge_copy(m - 2, h).wait_send()

            @pl.loop(0, half // min(CHUNK, half))
            def _(i):
                size = min(CHUNK, half)
                at = pl.ds(pl.multiple_of(i * size, size), size)
                total = own[slot, h, at].astype(F32) + mg[m % MG_SLOTS, h, 2, at].astype(F32)
                total = total + (mg[m % MG_SLOTS, h, 0, at].astype(F32) + mg[m % MG_SLOTS, h, 1, at].astype(F32))
                mout[m % 2, h, at] = total
            merge_copy(m, h).start()

        @pl.when(m + MG_SLOTS < n_mats)
        def _():
            for peer in peers:
                pl.semaphore_signal(s_free.at[m], inc=1, device_id={"data": peer}, device_id_type=MESH)

    def forward(m, h, near=True, distant=True):
        oc = owner_chip(m)
        late = m // chips
        wanted = oc != chip
        if not near:
            wanted = oc == far
        if not distant:
            wanted = wanted & (oc != far)
        src = fin.at[m, h, 0]
        dst = xin.at[late, pl.ds(pl.multiple_of(chip * rows + h * half, half), half)]

        if near:
            @pl.when(oc == chip)
            def _():
                pltpu.make_async_copy(src, dst, s_x.at[late, chip]).start()

        @pl.when(wanted)
        def _():
            remote(src, dst, s_xsend.at[m], s_x.at[late, chip], dev(oc, core)).start()

    def finish(m):
        slot = m % 3
        oc = owner_chip(m)
        late = m // chips
        wait_bytes(fin.at[m], s_fin.at[m])
        wait_bytes(momin.at[m % 2], s_mom.at[m % 2])
        size = min(CHUNK, half)
        acc = jnp.zeros((8, 128), F32)
        for h in range(2):
            wait_bytes(fsum.at[m, h], s_fsum.at[m, h], "wait_fsum")

            def part(i, acc):
                at = pl.ds(pl.multiple_of(i * size, size), size)
                mom_at = pl.ds(pl.multiple_of(h * half + i * size, size), size)
                total = own[slot, 2 + h, at].astype(F32) + fin[m, h, 2, at].astype(F32)
                total = total + (fin[m, h, 0, at].astype(F32) + fin[m, h, 1, at].astype(F32))
                total = total + fsum[m, h, at]
                new = MOMENTUM_COEF * momin[m % 2, mom_at] + total
                fsum[m, h, at] = new
                fin[m, h, 0, at] = new.astype(BF16)
                square = new * new
                for r in range(0, size, 8):
                    for q in range(0, cols, 128):
                        acc = acc + square[r:r + 8, q:q + 128]
                return acc

            acc = lax.fori_loop(0, half // size, part, acc)
            if h == 1:
                nsend[m] = acc
                sum_to = ninbox.at[late, me]

                @pl.when(oc == chip)
                def _():
                    pltpu.make_async_copy(nsend.at[m], sum_to, s_n.at[late]).start()
                    remote(nsend.at[m], sum_to, s_nsend.at[m], s_n.at[late], mate).start()

                @pl.when(oc != chip)
                def _():
                    for kk in range(CORES):
                        remote(nsend.at[m], sum_to, s_nsend.at[m], s_n.at[late], dev(oc, kk)).start()

            @pl.when((late == 0) | (m == n_mats - 1))
            def _():
                forward(m, h)

    first, second = pl.ds(0, hr), pl.ds(hr, hr)

    def to_mate(g, buf, at):
        return remote(buf.at[first, at], buf.at[second, at], s_xps.at[g], s_xp.at[g], mate)

    def ns_begin(e):
        g, buf = e * NS_ITERS, (xbuf0, xbuf1)[(e * NS_ITERS) % 2]
        wait_bytes(ninbox.at[e], s_n.at[e], "wait_n")
        total = jnp.sum(ninbox[e], axis=0)
        total = jnp.sum(jnp.sum(total, axis=0, keepdims=True), axis=1, keepdims=True)
        bound = jnp.sqrt(total) + NORM_EPS

        @pl.loop(0, chips)
        def _(step):
            away = jnp.where(step == 2, 3, jnp.where(step == 3, 2, step))
            b = (chip + away) % chips
            here = pl.ds(pl.multiple_of(b * rows, rows), rows)
            wait_bytes(xin.at[e, here], s_x.at[e, b], "wait_x")

            @pl.loop(0, rows // CHUNK)
            def _(i):
                at = pl.ds(pl.multiple_of(b * rows + i * CHUNK, CHUNK), CHUNK)
                buf[at] = (xin[e, at].astype(F32) / bound).astype(BF16)
            there = pl.ds(pl.multiple_of(hr + b * rows, rows), rows)
            remote(buf.at[here], buf.at[there], s_xps.at[g], s_xp.at[g], mate).start()

    def ns_iter(g, par, last, late):
        cur, nxt, col = ((xbuf0, xbuf1, colo0), (xbuf1, xbuf0, colo1))[par]
        transposed = (((1,), (1,)), ((), ()))
        diag = remote(row.at[:, first], col.at[second], s_aps.at[g], s_ap.at[g], mate)

        with jax.named_scope("gram"):
            prod = lax.dot_general(cur[first], cur[first], transposed, preferred_element_type=F32)
            row[:, first] = prod.astype(BF16)
            diag.start()
        wait_bytes(cur.at[second], s_xp.at[g], "wait_xp")
        with jax.named_scope("squares"):
            prod = lax.dot_general(cur[first], cur[second], transposed, preferred_element_type=F32)
            prod = prod.astype(BF16)
            row[:, second] = prod
            col[first] = prod
            prod = lax.dot_general(row[...], row[...], transposed, preferred_element_type=F32)
            poly[:, first] = (COEF_B * row[:, first].astype(F32) + COEF_C * prod).astype(BF16)
        wait_bytes(col.at[second], s_ap.at[g], "wait_ap")
        with jax.named_scope("newx"):
            prod = jnp.dot(row[...], col[...], preferred_element_type=F32)
            poly[:, second] = (COEF_B * row[:, second].astype(F32) + COEF_C * prod).astype(BF16)
            wide = cols // X_PARTS
            for j in range(X_PARTS):
                at = pl.ds(j * wide, wide)
                prod = jnp.dot(poly[...], cur[:, at], preferred_element_type=F32)
                nxt[first, at] = (COEF_A * cur[first, at].astype(F32) + prod).astype(BF16)
                if not last:
                    to_mate(g + 1, nxt, at).start()
                elif late:
                    give_back(1, nxt, at)
        if last and not late:
            keep = pltpu.make_async_copy(nxt.at[first], xin.at[0], s_keep)
            keep.start()
            keep.wait()
        diag.wait_send()
        wait_bytes(cur.at[first], s_xps.at[g])

    def give_back(e, src, at):
        mat = my_mat(e)
        dst = ret.at[mat, :, at]

        def block(c):
            return src.at[pl.ds(pl.multiple_of(c * rows, rows), rows), at]

        for i in range(1, chips):
            c = (chip + i) % chips
            remote(block(c), dst, s_rsend.at[e], s_ret.at[mat], dev(c, core)).start()
        pltpu.make_async_copy(block(chip), dst, s_ret.at[mat]).start()

    def early_done(s):
        return jnp.clip(ITERS_PER_STEP * (s - chip - 2), 0, NS_ITERS)

    barrier = pltpu.get_barrier_semaphore()
    for i in range(1, group):
        pl.semaphore_signal(barrier, inc=1, device_id={"data": (me + i) % group}, device_id_type=MESH)
    pl.semaphore_wait(barrier, group - 1)

    @pl.loop(0, AHEAD)
    def _(m):
        issue_raw(m)
    load_own(0)
    pltpu.make_async_copy(w_ref, wbuf, s_wload).start()

    @pl.loop(0, n_mats + 2)
    def _(s):
        @pl.when(s + AHEAD < n_mats)
        def _():
            issue_raw(s + AHEAD)

        @pl.when(s + 1 < n_mats)
        def _():
            load_own(s + 1)

        @pl.when(s < n_mats)
        def _():
            pltpu.make_async_copy(mom_ref.at[s], momin.at[s % 2], s_mom.at[s % 2]).start()
            merge(s)

        last = s == n_mats + 1
        lo = jnp.where(s >= n_mats, early_done(n_mats - 1), early_done(s - 1))
        hi = jnp.where(last, 2 * NS_ITERS, jnp.where(s >= n_mats, lo, early_done(s)))

        def run(g, carry):
            @pl.when(g == 0)
            def _():
                ns_begin(0)

            @pl.when(g == NS_ITERS)
            def _():
                ns_begin(1)

            @pl.when(g == NS_ITERS + HOLD)
            def _():
                give_back(0, xin.at[0], pl.ds(0, cols))

            end = g % NS_ITERS == NS_ITERS - 1
            for par in range(2):
                @pl.when((g % 2 == par) & jnp.logical_not(end))
                def _():
                    ns_iter(g, par, False, False)
            for e in range(2):
                @pl.when(g == (e + 1) * NS_ITERS - 1)
                def _():
                    ns_iter(g, ((e + 1) * NS_ITERS - 1) % 2, True, e == 1)
            return carry
        lax.fori_loop(lo, hi, run, 0)

        @pl.when((s >= 1) & (s <= n_mats))
        def _():
            finish(s - 1)

        for when, near in ((n_mats - 1, True), (n_mats, False)):
            @pl.when(s == when)
            def _():
                @pl.loop(chips, n_mats - 1)
                def _(m):
                    for h in range(2):
                        forward(m, h, near=near, distant=not near)

    wait_bytes(wbuf, s_wload)

    @pl.loop(0, n_mats)
    def _(m):
        done = g_ref.at[0, m, pl.ds(0, 12 * half)]
        wait_bytes(done, s_gsend.at[m])

        @pl.when(owner_chip(m) == chip)
        def _():
            wait_bytes(nsend.at[0], s_nsend.at[m])

        @pl.when(owner_chip(m) != chip)
        def _():
            wait_bytes(ret.at[m], s_xsend.at[m])
            wait_bytes(nsend.at[pl.ds(0, CORES)], s_nsend.at[m])
    for m in range(n_mats - 2, n_mats):
        for h in range(2):
            merge_copy(m, h).wait_send()

    @pl.loop(0, n_mats)
    def _(m):
        wait_bytes(ret.at[m], s_ret.at[m], "wait_ret")
    for e in range(2):
        wait_bytes(xin.at[e, pl.ds(0, (chips - 1) * rows)], s_rsend.at[e])


def finish_kernel(scale, w_ref, mom_ref, x_ref, w_out, mom_out, wnew, sem):
    n_mats, rows, _ = w_ref.shape
    copies = [pltpu.make_async_copy(mom_ref.at[pl.ds(m, 2)], mom_out.at[pl.ds(m, 2)], sem.at[m]) for m in range(0, n_mats, 2)]
    for copy in copies:
        copy.start()
    for m in range(n_mats):
        @pl.loop(0, rows // CHUNK)
        def _(i):
            at = pl.ds(pl.multiple_of(i * CHUNK, CHUNK), CHUNK)
            w = w_ref[m, at]
            wnew[m, at] = w - LEARN_RATE * (x_ref[m, at].astype(F32) * scale + WEIGHT_DECAY * w)
        copies.append(pltpu.make_async_copy(wnew.at[m], w_out.at[m], sem.at[n_mats + m]))
        copies[-1].start()
    for copy in copies:
        copy.wait()


def solution(mesh):
    group = mesh.shape['data']
    row_spec = P('stage', 'data', None)
    grad_spec = P(('stage', 'data'), None, None, None)

    def local_step(w_rows, mom_rows, grad_full):
        n_mats, rows, cols = w_rows.shape
        half = rows // 2
        n_rows = rows * group
        chips = group // CORES
        hr = n_rows // CORES
        scale = 0.2 * math.sqrt(max(n_rows, cols))
        hbm = pl.BlockSpec(memory_space=pl.ANY)
        vmem = pl.BlockSpec(memory_space=pltpu.VMEM)
        dma = pltpu.SemaphoreType.DMA
        flops = NS_ITERS * (4 * n_rows * n_rows * cols + 2 * n_rows ** 3)
        mom_new, w_held, x_rows = pl.pallas_call(
            functools.partial(fused_kernel, group),
            out_shape=(pltpu.VMEM((n_mats, 2, half, cols), F32), pltpu.VMEM(w_rows.shape, F32), pltpu.VMEM(w_rows.shape, BF16)),
            in_specs=[hbm] * 3,
            out_specs=(vmem, vmem, vmem),
            scratch_shapes=[
                pltpu.VMEM((MG_SLOTS, 2, 3, half, cols), BF16),
                pltpu.VMEM((n_mats, 2, 3, half, cols), BF16),
                pltpu.VMEM((3, 4, half, cols), BF16),
                pltpu.VMEM((2, 2, half, cols), F32),
                pltpu.VMEM((2, rows, cols), F32),
                pltpu.VMEM((2, hr, cols), BF16),
                pltpu.VMEM((n_rows, cols), BF16),
                pltpu.VMEM((n_rows, cols), BF16),
                pltpu.VMEM((hr, n_rows), BF16),
                pltpu.VMEM((n_rows, hr), BF16),
                pltpu.VMEM((n_rows, hr), BF16),
                pltpu.VMEM((hr, n_rows), BF16),
                pltpu.VMEM((n_mats, 8, 128), F32),
                pltpu.VMEM((2, group, 8, 128), F32),
                dma((n_mats, 2)), dma((n_mats,)), dma((n_mats, 2)), dma((3,)), dma((2, 2)), dma((2,)),
                dma((2, chips)), dma((2,)), dma((n_mats,)),
                dma((n_mats,)), dma((n_mats,)), dma((n_mats,)), dma((2,)), dma, pltpu.SemaphoreType.REGULAR((n_mats,)),
                dma((2 * NS_ITERS,)), dma((2 * NS_ITERS,)), dma((2 * NS_ITERS,)), dma((2 * NS_ITERS,)), dma,
            ],
            compiler_params=pltpu.CompilerParams(collective_id=0, has_side_effects=True, vmem_limit_bytes=43 * 2 ** 20),
            cost_estimate=pl.CostEstimate(flops=flops, bytes_accessed=2 ** 26, transcendentals=0),
            name="muon_step",
        )(w_rows, mom_rows, grad_full)
        mom_new = mom_new.reshape(w_rows.shape)
        return pl.pallas_call(
            functools.partial(finish_kernel, scale),
            out_shape=(jax.ShapeDtypeStruct(w_rows.shape, F32), jax.ShapeDtypeStruct(w_rows.shape, F32)),
            in_specs=[vmem] * 3,
            out_specs=(hbm, hbm),
            scratch_shapes=[pltpu.VMEM(w_rows.shape, F32), dma((2 * n_mats,))],
            compiler_params=pltpu.CompilerParams(vmem_limit_bytes=12 * 2 ** 20),
            cost_estimate=pl.CostEstimate(flops=4 * w_rows.size, bytes_accessed=2 * w_rows.size * 4, transcendentals=0),
            name="finish",
        )(w_held, mom_new, x_rows)

    return jax.shard_map(local_step, mesh=mesh, in_specs=(row_spec, row_spec, grad_spec), out_specs=(row_spec, row_spec), check_vma=False)
```

```python
import functools
import math
import jax
import jax.numpy as jnp
from jax import lax
from jax.experimental import pallas as pl
from jax.experimental.pallas import tpu as pltpu
from jax.sharding import PartitionSpec as P

MOMENTUM_COEF = 0.95
LEARN_RATE = 0.05
WEIGHT_DECAY = 0.2
NORM_EPS = 1e-7
COEF_A = 3.4445
COEF_B = -4.7750
COEF_C = 2.0315
NS_ITERS = 5

CORES = 2
AHEAD = 2
CHUNK = 32
ITERS_PER_STEP = 2
MG_SLOTS = 4
X_PARTS = 4
MESH = pl.DeviceIdType.MESH
F32 = jnp.float32
BF16 = jnp.bfloat16


def fused_kernel(group, w_ref, mom_ref, g_ref, fsum, wbuf, ret,
                 mg, fin, own, mout, momin, xin, xbuf0, xbuf1, row, colo0, colo1, poly, nsend, ninbox,
                 s_mg, s_fin, s_fsum, s_own, s_mout, s_mom, s_x, s_n, s_ret,
                 s_gsend, s_xsend, s_nsend, s_rsend, s_wload, s_free,
                 s_xp, s_xps, s_ap, s_aps, s_keep):
    n_mats, rows, cols = w_ref.shape
    half = rows // 2
    chips = group // CORES
    hr = rows * chips
    me = lax.axis_index("data")
    chip, core = me // CORES, me % CORES
    right, left, far = (chip + 1) % chips, (chip + chips - 1) % chips, (chip + 2) % chips

    def dev(a_chip, a_core):
        return a_chip * CORES + a_core

    mate = dev(chip, 1 - core)

    def owner_chip(m):
        return jnp.where(m < chips, m, 2 * chips - 1 - m)

    def my_mat(e):
        return jnp.where(e == 0, chip, 2 * chips - 1 - chip)

    def grad_rows(m, a_chip, a_core, h):
        start = pl.multiple_of(dev(a_chip, a_core) * rows + h * half, half)
        return g_ref.at[0, m, pl.ds(start, half)]

    def remote(src, dst, send, recv, to):
        return pltpu.make_async_remote_copy(src_ref=src, dst_ref=dst, send_sem=send, recv_sem=recv,
                                            device_id={"data": to}, device_id_type=MESH)

    def wait_bytes(ref, sem, name=None):
        if name is None:
            pltpu.make_async_copy(ref, ref, sem).wait()
        else:
            with jax.named_scope(name):
                pltpu.make_async_copy(ref, ref, sem).wait()

    peers = [dev(left, 0), dev(left, 1), dev(right, 0), dev(right, 1), mate]

    def issue_raw(m):
        send = s_gsend.at[m]

        @pl.when(m >= MG_SLOTS)
        def _():
            pl.semaphore_wait(s_free.at[jnp.maximum(m - MG_SLOTS, 0)], len(peers))
        for kk in range(CORES):
            remote(grad_rows(m, far, kk, 0), mg.at[m % MG_SLOTS, 0, core], send, s_mg.at[m % MG_SLOTS, 0], dev(right, kk)).start()
            remote(grad_rows(m, far, kk, 1), mg.at[m % MG_SLOTS, 1, core], send, s_mg.at[m % MG_SLOTS, 1], dev(left, kk)).start()
        remote(grad_rows(m, right, 1 - core, 0), mg.at[m % MG_SLOTS, 0, 2], send, s_mg.at[m % MG_SLOTS, 0], mate).start()
        remote(grad_rows(m, left, 1 - core, 1), mg.at[m % MG_SLOTS, 1, 2], send, s_mg.at[m % MG_SLOTS, 1], mate).start()
        for kk in range(CORES):
            remote(grad_rows(m, right, kk, 1), fin.at[m, 1, core], send, s_fin.at[m], dev(right, kk)).start()
            remote(grad_rows(m, left, kk, 0), fin.at[m, 0, core], send, s_fin.at[m], dev(left, kk)).start()
        for h in range(2):
            remote(grad_rows(m, chip, 1 - core, h), fin.at[m, h, 2], send, s_fin.at[m], mate).start()

    def load_own(m):
        slot = m % 3
        pltpu.make_async_copy(grad_rows(m, right, core, 0), own.at[slot, 0], s_own.at[slot]).start()
        pltpu.make_async_copy(grad_rows(m, left, core, 1), own.at[slot, 1], s_own.at[slot]).start()
        for h in range(2):
            pltpu.make_async_copy(grad_rows(m, chip, core, h), own.at[slot, 2 + h], s_own.at[slot]).start()

    def merge_copy(m, h):
        to = dev(right if h == 0 else left, core)
        return remote(mout.at[m % 2, h], fsum.at[m, h], s_mout.at[m % 2, h], s_fsum.at[m, h], to)

    def merge(m):
        slot = m % 3
        wait_bytes(own.at[slot], s_own.at[slot])
        for h in range(2):
            wait_bytes(mg.at[m % MG_SLOTS, h], s_mg.at[m % MG_SLOTS, h], "wait_mg")

            @pl.when(m >= 2)
            def _():
                merge_copy(m - 2, h).wait_send()

            @pl.loop(0, half // min(CHUNK, half))
            def _(i):
                size = min(CHUNK, half)
                at = pl.ds(pl.multiple_of(i * size, size), size)
                total = own[slot, h, at].astype(F32) + mg[m % MG_SLOTS, h, 2, at].astype(F32)
                total = total + (mg[m % MG_SLOTS, h, 0, at].astype(F32) + mg[m % MG_SLOTS, h, 1, at].astype(F32))
                mout[m % 2, h, at] = total
            merge_copy(m, h).start()

        @pl.when(m + MG_SLOTS < n_mats)
        def _():
            for peer in peers:
                pl.semaphore_signal(s_free.at[m], inc=1, device_id={"data": peer}, device_id_type=MESH)

    def forward(m, h, near=True, distant=True):
        oc = owner_chip(m)
        late = m // chips
        wanted = oc != chip
        if not near:
            wanted = oc == far
        if not distant:
            wanted = wanted & (oc != far)
        src = fin.at[m, h, 0]
        dst = xin.at[late, pl.ds(pl.multiple_of(chip * rows + h * half, half), half)]

        if near:
            @pl.when(oc == chip)
            def _():
                pltpu.make_async_copy(src, dst, s_x.at[late, chip]).start()

        @pl.when(wanted)
        def _():
            remote(src, dst, s_xsend.at[m], s_x.at[late, chip], dev(oc, core)).start()

    def finish(m):
        slot = m % 3
        oc = owner_chip(m)
        late = m // chips
        wait_bytes(fin.at[m], s_fin.at[m])
        wait_bytes(momin.at[m % 2], s_mom.at[m % 2])
        size = min(CHUNK, half)
        acc = jnp.zeros((8, 128), F32)
        for h in range(2):
            wait_bytes(fsum.at[m, h], s_fsum.at[m, h], "wait_fsum")

            def part(i, acc):
                at = pl.ds(pl.multiple_of(i * size, size), size)
                mom_at = pl.ds(pl.multiple_of(h * half + i * size, size), size)
                total = own[slot, 2 + h, at].astype(F32) + fin[m, h, 2, at].astype(F32)
                total = total + (fin[m, h, 0, at].astype(F32) + fin[m, h, 1, at].astype(F32))
                total = total + fsum[m, h, at]
                new = MOMENTUM_COEF * momin[m % 2, mom_at] + total
                fsum[m, h, at] = new
                fin[m, h, 0, at] = new.astype(BF16)
                square = new * new
                for r in range(0, size, 8):
                    for q in range(0, cols, 128):
                        acc = acc + square[r:r + 8, q:q + 128]
                return acc

            acc = lax.fori_loop(0, half // size, part, acc)
            if h == 1:
                nsend[m] = acc
                sum_to = ninbox.at[late, me]

                @pl.when(oc == chip)
                def _():
                    pltpu.make_async_copy(nsend.at[m], sum_to, s_n.at[late]).start()
                    remote(nsend.at[m], sum_to, s_nsend.at[m], s_n.at[late], mate).start()

                @pl.when(oc != chip)
                def _():
                    for kk in range(CORES):
                        remote(nsend.at[m], sum_to, s_nsend.at[m], s_n.at[late], dev(oc, kk)).start()

            @pl.when((late == 0) | (m == n_mats - 1))
            def _():
                forward(m, h)

    first, second = pl.ds(0, hr), pl.ds(hr, hr)

    def to_mate(g, buf, at):
        return remote(buf.at[first, at], buf.at[second, at], s_xps.at[g], s_xp.at[g], mate)

    def ns_begin(e):
        g, buf = e * NS_ITERS, (xbuf0, xbuf1)[(e * NS_ITERS) % 2]
        wait_bytes(ninbox.at[e], s_n.at[e], "wait_n")
        total = jnp.sum(ninbox[e], axis=0)
        total = jnp.sum(jnp.sum(total, axis=0, keepdims=True), axis=1, keepdims=True)
        bound = jnp.sqrt(total) + NORM_EPS

        @pl.loop(0, chips)
        def _(step):
            away = jnp.where(step == 2, 3, jnp.where(step == 3, 2, step))
            b = (chip + away) % chips
            here = pl.ds(pl.multiple_of(b * rows, rows), rows)
            wait_bytes(xin.at[e, here], s_x.at[e, b], "wait_x")

            @pl.loop(0, rows // CHUNK)
            def _(i):
                at = pl.ds(pl.multiple_of(b * rows + i * CHUNK, CHUNK), CHUNK)
                buf[at] = (xin[e, at].astype(F32) / bound).astype(BF16)
            there = pl.ds(pl.multiple_of(hr + b * rows, rows), rows)
            remote(buf.at[here], buf.at[there], s_xps.at[g], s_xp.at[g], mate).start()

    def ns_iter(g, par, last, late):
        cur, nxt, col = ((xbuf0, xbuf1, colo0), (xbuf1, xbuf0, colo1))[par]
        transposed = (((1,), (1,)), ((), ()))
        diag = remote(row.at[:, first], col.at[second], s_aps.at[g], s_ap.at[g], mate)

        with jax.named_scope("gram"):
            prod = lax.dot_general(cur[first], cur[first], transposed, preferred_element_type=F32)
            row[:, first] = prod.astype(BF16)
            diag.start()
        wait_bytes(cur.at[second], s_xp.at[g], "wait_xp")
        with jax.named_scope("squares"):
            prod = lax.dot_general(cur[first], cur[second], transposed, preferred_element_type=F32)
            prod = prod.astype(BF16)
            row[:, second] = prod
            col[first] = prod
            prod = lax.dot_general(row[...], row[...], transposed, preferred_element_type=F32)
            poly[:, first] = (COEF_B * row[:, first].astype(F32) + COEF_C * prod).astype(BF16)
        if par == NS_ITERS % 2 and not last:
            @pl.when(g == NS_ITERS)
            def _():
                give_back(0, xin.at[0], pl.ds(0, cols))
        wait_bytes(col.at[second], s_ap.at[g], "wait_ap")
        with jax.named_scope("newx"):
            prod = jnp.dot(row[...], col[...], preferred_element_type=F32)
            poly[:, second] = (COEF_B * row[:, second].astype(F32) + COEF_C * prod).astype(BF16)
            wide = cols // X_PARTS
            for j in range(X_PARTS):
                at = pl.ds(j * wide, wide)
                prod = jnp.dot(poly[...], cur[:, at], preferred_element_type=F32)
                nxt[first, at] = (COEF_A * cur[first, at].astype(F32) + prod).astype(BF16)
                if not last:
                    to_mate(g + 1, nxt, at).start()
                elif late:
                    give_back(1, nxt, at)
        if last and not late:
            keep = pltpu.make_async_copy(nxt.at[first], xin.at[0], s_keep)
            keep.start()
            keep.wait()
        diag.wait_send()
        wait_bytes(cur.at[first], s_xps.at[g])

    def give_back(e, src, at):
        mat = my_mat(e)
        dst = ret.at[mat, :, at]

        def block(c):
            return src.at[pl.ds(pl.multiple_of(c * rows, rows), rows), at]

        for i in range(1, chips):
            c = (chip + i) % chips
            remote(block(c), dst, s_rsend.at[e], s_ret.at[mat], dev(c, core)).start()
        pltpu.make_async_copy(block(chip), dst, s_ret.at[mat]).start()

    def early_done(s):
        return jnp.clip(ITERS_PER_STEP * (s - chip - 2), 0, NS_ITERS)

    barrier = pltpu.get_barrier_semaphore()
    for i in range(1, group):
        pl.semaphore_signal(barrier, inc=1, device_id={"data": (me + i) % group}, device_id_type=MESH)
    pl.semaphore_wait(barrier, group - 1)

    @pl.loop(0, AHEAD)
    def _(m):
        issue_raw(m)
    load_own(0)
    pltpu.make_async_copy(w_ref, wbuf, s_wload).start()

    @pl.loop(0, n_mats + 2)
    def _(s):
        @pl.when(s + AHEAD < n_mats)
        def _():
            issue_raw(s + AHEAD)

        @pl.when(s + 1 < n_mats)
        def _():
            load_own(s + 1)

        @pl.when(s < n_mats)
        def _():
            pltpu.make_async_copy(mom_ref.at[s], momin.at[s % 2], s_mom.at[s % 2]).start()
            merge(s)

        last = s == n_mats + 1
        lo = jnp.where(s >= n_mats, early_done(n_mats - 1), early_done(s - 1))
        hi = jnp.where(last, 2 * NS_ITERS, jnp.where(s >= n_mats, lo, early_done(s)))

        def run(g, carry):
            @pl.when(g == 0)
            def _():
                ns_begin(0)

            @pl.when(g == NS_ITERS)
            def _():
                ns_begin(1)

            end = g % NS_ITERS == NS_ITERS - 1
            for par in range(2):
                @pl.when((g % 2 == par) & jnp.logical_not(end))
                def _():
                    ns_iter(g, par, False, False)
            for e in range(2):
                @pl.when(g == (e + 1) * NS_ITERS - 1)
                def _():
                    ns_iter(g, ((e + 1) * NS_ITERS - 1) % 2, True, e == 1)
            return carry
        lax.fori_loop(lo, hi, run, 0)

        @pl.when((s >= 1) & (s <= n_mats))
        def _():
            finish(s - 1)

        for when, near in ((n_mats - 1, True), (n_mats, False)):
            @pl.when(s == when)
            def _():
                @pl.loop(chips, n_mats - 1)
                def _(m):
                    for h in range(2):
                        forward(m, h, near=near, distant=not near)

    wait_bytes(wbuf, s_wload)

    @pl.loop(0, n_mats)
    def _(m):
        done = g_ref.at[0, m, pl.ds(0, 12 * half)]
        wait_bytes(done, s_gsend.at[m])

        @pl.when(owner_chip(m) == chip)
        def _():
            wait_bytes(nsend.at[0], s_nsend.at[m])

        @pl.when(owner_chip(m) != chip)
        def _():
            wait_bytes(ret.at[m], s_xsend.at[m])
            wait_bytes(nsend.at[pl.ds(0, CORES)], s_nsend.at[m])
    for m in range(n_mats - 2, n_mats):
        for h in range(2):
            merge_copy(m, h).wait_send()

    @pl.loop(0, n_mats)
    def _(m):
        wait_bytes(ret.at[m], s_ret.at[m], "wait_ret")
    for e in range(2):
        wait_bytes(xin.at[e, pl.ds(0, (chips - 1) * rows)], s_rsend.at[e])


def finish_kernel(scale, w_ref, mom_ref, x_ref, w_out, mom_out, wnew, sem):
    n_mats, rows, _ = w_ref.shape
    copies = [pltpu.make_async_copy(mom_ref.at[pl.ds(m, 2)], mom_out.at[pl.ds(m, 2)], sem.at[m]) for m in range(0, n_mats, 2)]
    for copy in copies:
        copy.start()
    for m in range(n_mats):
        @pl.loop(0, rows // CHUNK)
        def _(i):
            at = pl.ds(pl.multiple_of(i * CHUNK, CHUNK), CHUNK)
            w = w_ref[m, at]
            wnew[m, at] = w - LEARN_RATE * (x_ref[m, at].astype(F32) * scale + WEIGHT_DECAY * w)
        copies.append(pltpu.make_async_copy(wnew.at[m], w_out.at[m], sem.at[n_mats + m]))
        copies[-1].start()
    for copy in copies:
        copy.wait()


def solution(mesh):
    group = mesh.shape['data']
    row_spec = P('stage', 'data', None)
    grad_spec = P(('stage', 'data'), None, None, None)

    def local_step(w_rows, mom_rows, grad_full):
        n_mats, rows, cols = w_rows.shape
        half = rows // 2
        n_rows = rows * group
        chips = group // CORES
        hr = n_rows // CORES
        scale = 0.2 * math.sqrt(max(n_rows, cols))
        hbm = pl.BlockSpec(memory_space=pl.ANY)
        vmem = pl.BlockSpec(memory_space=pltpu.VMEM)
        dma = pltpu.SemaphoreType.DMA
        flops = NS_ITERS * (4 * n_rows * n_rows * cols + 2 * n_rows ** 3)
        mom_new, w_held, x_rows = pl.pallas_call(
            functools.partial(fused_kernel, group),
            out_shape=(pltpu.VMEM((n_mats, 2, half, cols), F32), pltpu.VMEM(w_rows.shape, F32), pltpu.VMEM(w_rows.shape, BF16)),
            in_specs=[hbm] * 3,
            out_specs=(vmem, vmem, vmem),
            scratch_shapes=[
                pltpu.VMEM((MG_SLOTS, 2, 3, half, cols), BF16),
                pltpu.VMEM((n_mats, 2, 3, half, cols), BF16),
                pltpu.VMEM((3, 4, half, cols), BF16),
                pltpu.VMEM((2, 2, half, cols), F32),
                pltpu.VMEM((2, rows, cols), F32),
                pltpu.VMEM((2, hr, cols), BF16),
                pltpu.VMEM((n_rows, cols), BF16),
                pltpu.VMEM((n_rows, cols), BF16),
                pltpu.VMEM((hr, n_rows), BF16),
                pltpu.VMEM((n_rows, hr), BF16),
                pltpu.VMEM((n_rows, hr), BF16),
                pltpu.VMEM((hr, n_rows), BF16),
                pltpu.VMEM((n_mats, 8, 128), F32),
                pltpu.VMEM((2, group, 8, 128), F32),
                dma((n_mats, 2)), dma((n_mats,)), dma((n_mats, 2)), dma((3,)), dma((2, 2)), dma((2,)),
                dma((2, chips)), dma((2,)), dma((n_mats,)),
                dma((n_mats,)), dma((n_mats,)), dma((n_mats,)), dma((2,)), dma, pltpu.SemaphoreType.REGULAR((n_mats,)),
                dma((2 * NS_ITERS,)), dma((2 * NS_ITERS,)), dma((2 * NS_ITERS,)), dma((2 * NS_ITERS,)), dma,
            ],
            compiler_params=pltpu.CompilerParams(collective_id=0, has_side_effects=True, vmem_limit_bytes=43 * 2 ** 20),
            cost_estimate=pl.CostEstimate(flops=flops, bytes_accessed=2 ** 26, transcendentals=0),
            name="muon_step",
        )(w_rows, mom_rows, grad_full)
        mom_new = mom_new.reshape(w_rows.shape)
        return pl.pallas_call(
            functools.partial(finish_kernel, scale),
            out_shape=(jax.ShapeDtypeStruct(w_rows.shape, F32), jax.ShapeDtypeStruct(w_rows.shape, F32)),
            in_specs=[vmem] * 3,
            out_specs=(hbm, hbm),
            scratch_shapes=[pltpu.VMEM(w_rows.shape, F32), dma((2 * n_mats,))],
            compiler_params=pltpu.CompilerParams(vmem_limit_bytes=12 * 2 ** 20),
            cost_estimate=pl.CostEstimate(flops=4 * w_rows.size, bytes_accessed=2 * w_rows.size * 4, transcendentals=0),
            name="finish",
        )(w_held, mom_new, x_rows)

    return jax.shard_map(local_step, mesh=mesh, in_specs=(row_spec, row_spec, grad_spec), out_specs=(row_spec, row_spec), check_vma=False)
```

```python
import functools
import math
import jax
import jax.numpy as jnp
from jax import lax
from jax.experimental import pallas as pl
from jax.experimental.pallas import tpu as pltpu
from jax.sharding import PartitionSpec as P

MOMENTUM_COEF = 0.95
LEARN_RATE = 0.05
WEIGHT_DECAY = 0.2
NORM_EPS = 1e-7
COEF_A = 3.4445
COEF_B = -4.7750
COEF_C = 2.0315
NS_ITERS = 5

CORES = 2
AHEAD = 2
NEAR, FAR = (1, 3, 0), (2,)
CHUNK = 32
ITERS_PER_STEP = 2
MG_SLOTS = 4
X_PARTS = 4
MESH = pl.DeviceIdType.MESH
F32 = jnp.float32
BF16 = jnp.bfloat16


def fused_kernel(group, w_ref, mom_ref, g_ref, fsum, wbuf, ret,
                 mg, fin, own, mout, momin, xin, xbuf0, xbuf1, row, colo0, colo1, poly, nsend, ninbox,
                 s_mg, s_fin, s_fsum, s_own, s_mout, s_mom, s_x, s_n, s_ret,
                 s_gsend, s_xsend, s_nsend, s_rsend, s_wload, s_free,
                 s_xp, s_xps, s_ap, s_aps, s_keep):
    n_mats, rows, cols = w_ref.shape
    half = rows // 2
    chips = group // CORES
    hr = rows * chips
    me = lax.axis_index("data")
    chip, core = me // CORES, me % CORES
    right, left, far = (chip + 1) % chips, (chip + chips - 1) % chips, (chip + 2) % chips

    def dev(a_chip, a_core):
        return a_chip * CORES + a_core

    mate = dev(chip, 1 - core)

    def owner_chip(m):
        return jnp.where(m < chips, m, 2 * chips - 1 - m)

    def my_mat(e):
        return jnp.where(e == 0, chip, 2 * chips - 1 - chip)

    def grad_rows(m, a_chip, a_core, h):
        start = pl.multiple_of(dev(a_chip, a_core) * rows + h * half, half)
        return g_ref.at[0, m, pl.ds(start, half)]

    def remote(src, dst, send, recv, to):
        return pltpu.make_async_remote_copy(src_ref=src, dst_ref=dst, send_sem=send, recv_sem=recv,
                                            device_id={"data": to}, device_id_type=MESH)

    def wait_bytes(ref, sem, name=None):
        if name is None:
            pltpu.make_async_copy(ref, ref, sem).wait()
        else:
            with jax.named_scope(name):
                pltpu.make_async_copy(ref, ref, sem).wait()

    peers = [dev(left, 0), dev(left, 1), dev(right, 0), dev(right, 1), mate]

    def issue_raw(m):
        send = s_gsend.at[m]

        @pl.when(m >= MG_SLOTS)
        def _():
            pl.semaphore_wait(s_free.at[jnp.maximum(m - MG_SLOTS, 0)], len(peers))
        for kk in range(CORES):
            remote(grad_rows(m, far, kk, 0), mg.at[m % MG_SLOTS, 0, core], send, s_mg.at[m % MG_SLOTS, 0], dev(right, kk)).start()
            remote(grad_rows(m, far, kk, 1), mg.at[m % MG_SLOTS, 1, core], send, s_mg.at[m % MG_SLOTS, 1], dev(left, kk)).start()
        remote(grad_rows(m, right, 1 - core, 0), mg.at[m % MG_SLOTS, 0, 2], send, s_mg.at[m % MG_SLOTS, 0], mate).start()
        remote(grad_rows(m, left, 1 - core, 1), mg.at[m % MG_SLOTS, 1, 2], send, s_mg.at[m % MG_SLOTS, 1], mate).start()
        for kk in range(CORES):
            remote(grad_rows(m, right, kk, 1), fin.at[m, 1, core], send, s_fin.at[m], dev(right, kk)).start()
            remote(grad_rows(m, left, kk, 0), fin.at[m, 0, core], send, s_fin.at[m], dev(left, kk)).start()
        for h in range(2):
            remote(grad_rows(m, chip, 1 - core, h), fin.at[m, h, 2], send, s_fin.at[m], mate).start()

    def load_own(m):
        slot = m % 3
        pltpu.make_async_copy(grad_rows(m, right, core, 0), own.at[slot, 0], s_own.at[slot]).start()
        pltpu.make_async_copy(grad_rows(m, left, core, 1), own.at[slot, 1], s_own.at[slot]).start()
        for h in range(2):
            pltpu.make_async_copy(grad_rows(m, chip, core, h), own.at[slot, 2 + h], s_own.at[slot]).start()

    def merge_copy(m, h):
        to = dev(right if h == 0 else left, core)
        return remote(mout.at[m % 2, h], fsum.at[m, h], s_mout.at[m % 2, h], s_fsum.at[m, h], to)

    def merge(m):
        slot = m % 3
        wait_bytes(own.at[slot], s_own.at[slot])
        for h in range(2):
            wait_bytes(mg.at[m % MG_SLOTS, h], s_mg.at[m % MG_SLOTS, h], "wait_mg")

            @pl.when(m >= 2)
            def _():
                merge_copy(m - 2, h).wait_send()

            @pl.loop(0, half // min(CHUNK, half))
            def _(i):
                size = min(CHUNK, half)
                at = pl.ds(pl.multiple_of(i * size, size), size)
                total = own[slot, h, at].astype(F32) + mg[m % MG_SLOTS, h, 2, at].astype(F32)
                total = total + (mg[m % MG_SLOTS, h, 0, at].astype(F32) + mg[m % MG_SLOTS, h, 1, at].astype(F32))
                mout[m % 2, h, at] = total
            merge_copy(m, h).start()

        @pl.when(m + MG_SLOTS < n_mats)
        def _():
            for peer in peers:
                pl.semaphore_signal(s_free.at[m], inc=1, device_id={"data": peer}, device_id_type=MESH)

    def forward(m, h, near=True, distant=True):
        oc = owner_chip(m)
        late = m // chips
        wanted = oc != chip
        if not near:
            wanted = oc == far
        if not distant:
            wanted = wanted & (oc != far)
        src = fin.at[m, h, 0]
        dst = xin.at[late, pl.ds(pl.multiple_of(chip * rows + h * half, half), half)]

        if near:
            @pl.when(oc == chip)
            def _():
                pltpu.make_async_copy(src, dst, s_x.at[late, chip]).start()

        @pl.when(wanted)
        def _():
            remote(src, dst, s_xsend.at[m], s_x.at[late, chip], dev(oc, core)).start()

    def finish(m):
        slot = m % 3
        oc = owner_chip(m)
        late = m // chips
        wait_bytes(fin.at[m], s_fin.at[m])
        wait_bytes(momin.at[m % 2], s_mom.at[m % 2])
        size = min(CHUNK, half)
        acc = jnp.zeros((8, 128), F32)
        for h in range(2):
            wait_bytes(fsum.at[m, h], s_fsum.at[m, h], "wait_fsum")

            def part(i, acc):
                at = pl.ds(pl.multiple_of(i * size, size), size)
                mom_at = pl.ds(pl.multiple_of(h * half + i * size, size), size)
                total = own[slot, 2 + h, at].astype(F32) + fin[m, h, 2, at].astype(F32)
                total = total + (fin[m, h, 0, at].astype(F32) + fin[m, h, 1, at].astype(F32))
                total = total + fsum[m, h, at]
                new = MOMENTUM_COEF * momin[m % 2, mom_at] + total
                fsum[m, h, at] = new
                fin[m, h, 0, at] = new.astype(BF16)
                square = new * new
                for r in range(0, size, 8):
                    for q in range(0, cols, 128):
                        acc = acc + square[r:r + 8, q:q + 128]
                return acc

            acc = lax.fori_loop(0, half // size, part, acc)
            if h == 1:
                nsend[m] = acc
                sum_to = ninbox.at[late, me]

                @pl.when(oc == chip)
                def _():
                    pltpu.make_async_copy(nsend.at[m], sum_to, s_n.at[late]).start()
                    remote(nsend.at[m], sum_to, s_nsend.at[m], s_n.at[late], mate).start()

                @pl.when(oc != chip)
                def _():
                    for kk in range(CORES):
                        remote(nsend.at[m], sum_to, s_nsend.at[m], s_n.at[late], dev(oc, kk)).start()

            @pl.when((late == 0) | (m == n_mats - 1))
            def _():
                forward(m, h)

    first, second = pl.ds(0, hr), pl.ds(hr, hr)

    def to_mate(g, buf, at):
        return remote(buf.at[first, at], buf.at[second, at], s_xps.at[g], s_xp.at[g], mate)

    def ns_begin(e):
        g, buf = e * NS_ITERS, (xbuf0, xbuf1)[(e * NS_ITERS) % 2]
        wait_bytes(ninbox.at[e], s_n.at[e], "wait_n")
        total = jnp.sum(ninbox[e], axis=0)
        total = jnp.sum(jnp.sum(total, axis=0, keepdims=True), axis=1, keepdims=True)
        bound = jnp.sqrt(total) + NORM_EPS

        @pl.loop(0, chips)
        def _(step):
            away = jnp.where(step == 2, 3, jnp.where(step == 3, 2, step))
            b = (chip + away) % chips
            here = pl.ds(pl.multiple_of(b * rows, rows), rows)
            wait_bytes(xin.at[e, here], s_x.at[e, b], "wait_x")

            @pl.loop(0, rows // CHUNK)
            def _(i):
                at = pl.ds(pl.multiple_of(b * rows + i * CHUNK, CHUNK), CHUNK)
                buf[at] = (xin[e, at].astype(F32) / bound).astype(BF16)
            there = pl.ds(pl.multiple_of(hr + b * rows, rows), rows)
            remote(buf.at[here], buf.at[there], s_xps.at[g], s_xp.at[g], mate).start()

    def ns_iter(g, par, last, late):
        cur, nxt, col = ((xbuf0, xbuf1, colo0), (xbuf1, xbuf0, colo1))[par]
        transposed = (((1,), (1,)), ((), ()))
        diag = remote(row.at[:, first], col.at[second], s_aps.at[g], s_ap.at[g], mate)

        with jax.named_scope("gram"):
            prod = lax.dot_general(cur[first], cur[first], transposed, preferred_element_type=F32)
            row[:, first] = prod.astype(BF16)
            diag.start()
        wait_bytes(cur.at[second], s_xp.at[g], "wait_xp")
        with jax.named_scope("squares"):
            prod = lax.dot_general(cur[first], cur[second], transposed, preferred_element_type=F32)
            prod = prod.astype(BF16)
            row[:, second] = prod
            col[first] = prod
            prod = lax.dot_general(row[...], row[...], transposed, preferred_element_type=F32)
            poly[:, first] = (COEF_B * row[:, first].astype(F32) + COEF_C * prod).astype(BF16)
        if par == NS_ITERS % 2 and not last:
            @pl.when(g == NS_ITERS)
            def _():
                give_back(0, xin.at[0], pl.ds(0, cols), NEAR + FAR)
        wait_bytes(col.at[second], s_ap.at[g], "wait_ap")
        with jax.named_scope("newx"):
            prod = jnp.dot(row[...], col[...], preferred_element_type=F32)
            poly[:, second] = (COEF_B * row[:, second].astype(F32) + COEF_C * prod).astype(BF16)
            wide = cols // X_PARTS
            for j in range(X_PARTS):
                at = pl.ds(j * wide, wide)
                prod = jnp.dot(poly[...], cur[:, at], preferred_element_type=F32)
                nxt[first, at] = (COEF_A * cur[first, at].astype(F32) + prod).astype(BF16)
                if not last:
                    to_mate(g + 1, nxt, at).start()
                elif late:
                    give_back(1, nxt, at, NEAR)
            if late:
                give_back(1, nxt, pl.ds(0, cols), FAR)
        if last and not late:
            keep = pltpu.make_async_copy(nxt.at[first], xin.at[0], s_keep)
            keep.start()
            keep.wait()
        diag.wait_send()
        wait_bytes(cur.at[first], s_xps.at[g])

    def give_back(e, src, at, steps):
        mat = my_mat(e)
        dst = ret.at[mat, :, at]

        def block(c):
            return src.at[pl.ds(pl.multiple_of(c * rows, rows), rows), at]

        for i in steps:
            c = (chip + i) % chips
            if i == 0:
                pltpu.make_async_copy(block(chip), dst, s_ret.at[mat]).start()
            else:
                remote(block(c), dst, s_rsend.at[e], s_ret.at[mat], dev(c, core)).start()

    def early_done(s):
        return jnp.clip(ITERS_PER_STEP * (s - chip - 2), 0, NS_ITERS)

    barrier = pltpu.get_barrier_semaphore()
    for i in range(1, group):
        pl.semaphore_signal(barrier, inc=1, device_id={"data": (me + i) % group}, device_id_type=MESH)
    pl.semaphore_wait(barrier, group - 1)

    @pl.loop(0, AHEAD)
    def _(m):
        issue_raw(m)
    load_own(0)
    pltpu.make_async_copy(w_ref, wbuf, s_wload).start()

    @pl.loop(0, n_mats + 2)
    def _(s):
        @pl.when(s + AHEAD < n_mats)
        def _():
            issue_raw(s + AHEAD)

        @pl.when(s + 1 < n_mats)
        def _():
            load_own(s + 1)

        @pl.when(s < n_mats)
        def _():
            pltpu.make_async_copy(mom_ref.at[s], momin.at[s % 2], s_mom.at[s % 2]).start()
            merge(s)

        last = s == n_mats + 1
        lo = jnp.where(s >= n_mats, early_done(n_mats - 1), early_done(s - 1))
        hi = jnp.where(last, 2 * NS_ITERS, jnp.where(s >= n_mats, lo, early_done(s)))

        def run(g, carry):
            @pl.when(g == 0)
            def _():
                ns_begin(0)

            @pl.when(g == NS_ITERS)
            def _():
                ns_begin(1)

            end = g % NS_ITERS == NS_ITERS - 1
            for par in range(2):
                @pl.when((g % 2 == par) & jnp.logical_not(end))
                def _():
                    ns_iter(g, par, False, False)
            for e in range(2):
                @pl.when(g == (e + 1) * NS_ITERS - 1)
                def _():
                    ns_iter(g, ((e + 1) * NS_ITERS - 1) % 2, True, e == 1)
            return carry
        lax.fori_loop(lo, hi, run, 0)

        @pl.when((s >= 1) & (s <= n_mats))
        def _():
            finish(s - 1)

        for when, near in ((n_mats - 1, True), (n_mats, False)):
            @pl.when(s == when)
            def _():
                @pl.loop(chips, n_mats - 1)
                def _(m):
                    for h in range(2):
                        forward(m, h, near=near, distant=not near)

    wait_bytes(wbuf, s_wload)

    @pl.loop(0, n_mats)
    def _(m):
        done = g_ref.at[0, m, pl.ds(0, 12 * half)]
        wait_bytes(done, s_gsend.at[m])

        @pl.when(owner_chip(m) == chip)
        def _():
            wait_bytes(nsend.at[0], s_nsend.at[m])

        @pl.when(owner_chip(m) != chip)
        def _():
            wait_bytes(ret.at[m], s_xsend.at[m])
            wait_bytes(nsend.at[pl.ds(0, CORES)], s_nsend.at[m])
    for m in range(n_mats - 2, n_mats):
        for h in range(2):
            merge_copy(m, h).wait_send()

    @pl.loop(0, n_mats)
    def _(m):
        wait_bytes(ret.at[m], s_ret.at[m], "wait_ret")
    for e in range(2):
        wait_bytes(xin.at[e, pl.ds(0, (chips - 1) * rows)], s_rsend.at[e])


def finish_kernel(scale, w_ref, mom_ref, x_ref, w_out, mom_out, wnew, sem):
    n_mats, rows, _ = w_ref.shape
    copies = [pltpu.make_async_copy(mom_ref.at[pl.ds(m, 2)], mom_out.at[pl.ds(m, 2)], sem.at[m]) for m in range(0, n_mats, 2)]
    for copy in copies:
        copy.start()
    for m in range(n_mats):
        @pl.loop(0, rows // CHUNK)
        def _(i):
            at = pl.ds(pl.multiple_of(i * CHUNK, CHUNK), CHUNK)
            w = w_ref[m, at]
            wnew[m, at] = w - LEARN_RATE * (x_ref[m, at].astype(F32) * scale + WEIGHT_DECAY * w)
        copies.append(pltpu.make_async_copy(wnew.at[m], w_out.at[m], sem.at[n_mats + m]))
        copies[-1].start()
    for copy in copies:
        copy.wait()


def solution(mesh):
    group = mesh.shape['data']
    row_spec = P('stage', 'data', None)
    grad_spec = P(('stage', 'data'), None, None, None)

    def local_step(w_rows, mom_rows, grad_full):
        n_mats, rows, cols = w_rows.shape
        half = rows // 2
        n_rows = rows * group
        chips = group // CORES
        hr = n_rows // CORES
        scale = 0.2 * math.sqrt(max(n_rows, cols))
        hbm = pl.BlockSpec(memory_space=pl.ANY)
        vmem = pl.BlockSpec(memory_space=pltpu.VMEM)
        dma = pltpu.SemaphoreType.DMA
        flops = NS_ITERS * (4 * n_rows * n_rows * cols + 2 * n_rows ** 3)
        mom_new, w_held, x_rows = pl.pallas_call(
            functools.partial(fused_kernel, group),
            out_shape=(pltpu.VMEM((n_mats, 2, half, cols), F32), pltpu.VMEM(w_rows.shape, F32), pltpu.VMEM(w_rows.shape, BF16)),
            in_specs=[hbm] * 3,
            out_specs=(vmem, vmem, vmem),
            scratch_shapes=[
                pltpu.VMEM((MG_SLOTS, 2, 3, half, cols), BF16),
                pltpu.VMEM((n_mats, 2, 3, half, cols), BF16),
                pltpu.VMEM((3, 4, half, cols), BF16),
                pltpu.VMEM((2, 2, half, cols), F32),
                pltpu.VMEM((2, rows, cols), F32),
                pltpu.VMEM((2, hr, cols), BF16),
                pltpu.VMEM((n_rows, cols), BF16),
                pltpu.VMEM((n_rows, cols), BF16),
                pltpu.VMEM((hr, n_rows), BF16),
                pltpu.VMEM((n_rows, hr), BF16),
                pltpu.VMEM((n_rows, hr), BF16),
                pltpu.VMEM((hr, n_rows), BF16),
                pltpu.VMEM((n_mats, 8, 128), F32),
                pltpu.VMEM((2, group, 8, 128), F32),
                dma((n_mats, 2)), dma((n_mats,)), dma((n_mats, 2)), dma((3,)), dma((2, 2)), dma((2,)),
                dma((2, chips)), dma((2,)), dma((n_mats,)),
                dma((n_mats,)), dma((n_mats,)), dma((n_mats,)), dma((2,)), dma, pltpu.SemaphoreType.REGULAR((n_mats,)),
                dma((2 * NS_ITERS,)), dma((2 * NS_ITERS,)), dma((2 * NS_ITERS,)), dma((2 * NS_ITERS,)), dma,
            ],
            compiler_params=pltpu.CompilerParams(collective_id=0, has_side_effects=True, vmem_limit_bytes=43 * 2 ** 20),
            cost_estimate=pl.CostEstimate(flops=flops, bytes_accessed=2 ** 26, transcendentals=0),
            name="muon_step",
        )(w_rows, mom_rows, grad_full)
        mom_new = mom_new.reshape(w_rows.shape)
        return pl.pallas_call(
            functools.partial(finish_kernel, scale),
            out_shape=(jax.ShapeDtypeStruct(w_rows.shape, F32), jax.ShapeDtypeStruct(w_rows.shape, F32)),
            in_specs=[vmem] * 3,
            out_specs=(hbm, hbm),
            scratch_shapes=[pltpu.VMEM(w_rows.shape, F32), dma((2 * n_mats,))],
            compiler_params=pltpu.CompilerParams(vmem_limit_bytes=12 * 2 ** 20),
            cost_estimate=pl.CostEstimate(flops=4 * w_rows.size, bytes_accessed=2 * w_rows.size * 4, transcendentals=0),
            name="finish",
        )(w_held, mom_new, x_rows)

    return jax.shard_map(local_step, mesh=mesh, in_specs=(row_spec, row_spec, grad_spec), out_specs=(row_spec, row_spec), check_vma=False)
```

```python
import functools
import math
import jax
import jax.numpy as jnp
from jax import lax
from jax.experimental import pallas as pl
from jax.experimental.pallas import tpu as pltpu
from jax.sharding import PartitionSpec as P

MOMENTUM_COEF = 0.95
LEARN_RATE = 0.05
WEIGHT_DECAY = 0.2
NORM_EPS = 1e-7
COEF_A = 3.4445
COEF_B = -4.7750
COEF_C = 2.0315
NS_ITERS = 5

CORES = 2
AHEAD = 2
CHUNK = 32
ITERS_PER_STEP = 2
MG_SLOTS = 4
X_PARTS = 4
MESH = pl.DeviceIdType.MESH
F32 = jnp.float32
BF16 = jnp.bfloat16


def fused_kernel(group, w_ref, mom_ref, g_ref, fsum, wbuf, ret,
                 mg, fin, own, mout, momin, xin, xbuf0, xbuf1, row, colo0, colo1, poly, nsend, ninbox,
                 s_mg, s_fin, s_fsum, s_own, s_mout, s_mom, s_x, s_n, s_ret,
                 s_gsend, s_xsend, s_nsend, s_rsend, s_wload, s_free,
                 s_xp, s_xps, s_ap, s_aps, s_keep):
    n_mats, rows, cols = w_ref.shape
    half = rows // 2
    chips = group // CORES
    hr = rows * chips
    me = lax.axis_index("data")
    chip, core = me // CORES, me % CORES
    right, left, far = (chip + 1) % chips, (chip + chips - 1) % chips, (chip + 2) % chips

    def dev(a_chip, a_core):
        return a_chip * CORES + a_core

    mate = dev(chip, 1 - core)

    def owner_chip(m):
        return jnp.where(m < chips, m, (m + chips - 1) % chips)

    def my_mat(e):
        return jnp.where(e == 0, chip, chips + (chip + 1) % chips)

    def grad_rows(m, a_chip, a_core, h):
        start = pl.multiple_of(dev(a_chip, a_core) * rows + h * half, half)
        return g_ref.at[0, m, pl.ds(start, half)]

    def remote(src, dst, send, recv, to):
        return pltpu.make_async_remote_copy(src_ref=src, dst_ref=dst, send_sem=send, recv_sem=recv,
                                            device_id={"data": to}, device_id_type=MESH)

    def wait_bytes(ref, sem, name=None):
        if name is None:
            pltpu.make_async_copy(ref, ref, sem).wait()
        else:
            with jax.named_scope(name):
                pltpu.make_async_copy(ref, ref, sem).wait()

    peers = [dev(left, 0), dev(left, 1), dev(right, 0), dev(right, 1), mate]

    def issue_raw(m):
        send = s_gsend.at[m]

        @pl.when(m >= MG_SLOTS)
        def _():
            pl.semaphore_wait(s_free.at[jnp.maximum(m - MG_SLOTS, 0)], len(peers))
        for kk in range(CORES):
            remote(grad_rows(m, far, kk, 0), mg.at[m % MG_SLOTS, 0, core], send, s_mg.at[m % MG_SLOTS, 0], dev(right, kk)).start()
            remote(grad_rows(m, far, kk, 1), mg.at[m % MG_SLOTS, 1, core], send, s_mg.at[m % MG_SLOTS, 1], dev(left, kk)).start()
        remote(grad_rows(m, right, 1 - core, 0), mg.at[m % MG_SLOTS, 0, 2], send, s_mg.at[m % MG_SLOTS, 0], mate).start()
        remote(grad_rows(m, left, 1 - core, 1), mg.at[m % MG_SLOTS, 1, 2], send, s_mg.at[m % MG_SLOTS, 1], mate).start()
        for kk in range(CORES):
            remote(grad_rows(m, right, kk, 1), fin.at[m, 1, core], send, s_fin.at[m], dev(right, kk)).start()
            remote(grad_rows(m, left, kk, 0), fin.at[m, 0, core], send, s_fin.at[m], dev(left, kk)).start()
        for h in range(2):
            remote(grad_rows(m, chip, 1 - core, h), fin.at[m, h, 2], send, s_fin.at[m], mate).start()

    def load_own(m):
        slot = m % 3
        pltpu.make_async_copy(grad_rows(m, right, core, 0), own.at[slot, 0], s_own.at[slot]).start()
        pltpu.make_async_copy(grad_rows(m, left, core, 1), own.at[slot, 1], s_own.at[slot]).start()
        for h in range(2):
            pltpu.make_async_copy(grad_rows(m, chip, core, h), own.at[slot, 2 + h], s_own.at[slot]).start()

    def merge_copy(m, h):
        to = dev(right if h == 0 else left, core)
        return remote(mout.at[m % 2, h], fsum.at[m, h], s_mout.at[m % 2, h], s_fsum.at[m, h], to)

    def merge(m):
        slot = m % 3
        wait_bytes(own.at[slot], s_own.at[slot])
        for h in range(2):
            wait_bytes(mg.at[m % MG_SLOTS, h], s_mg.at[m % MG_SLOTS, h], "wait_mg")

            @pl.when(m >= 2)
            def _():
                merge_copy(m - 2, h).wait_send()

            @pl.loop(0, half // min(CHUNK, half))
            def _(i):
                size = min(CHUNK, half)
                at = pl.ds(pl.multiple_of(i * size, size), size)
                total = own[slot, h, at].astype(F32) + mg[m % MG_SLOTS, h, 2, at].astype(F32)
                total = total + (mg[m % MG_SLOTS, h, 0, at].astype(F32) + mg[m % MG_SLOTS, h, 1, at].astype(F32))
                mout[m % 2, h, at] = total
            merge_copy(m, h).start()

        @pl.when(m + MG_SLOTS < n_mats)
        def _():
            for peer in peers:
                pl.semaphore_signal(s_free.at[m], inc=1, device_id={"data": peer}, device_id_type=MESH)

    def forward(m, h, near=True, distant=True):
        oc = owner_chip(m)
        late = m // chips
        wanted = oc != chip
        if not near:
            wanted = oc == far
        if not distant:
            wanted = wanted & (oc != far)
        src = fin.at[m, h, 0]
        dst = xin.at[late, pl.ds(pl.multiple_of(chip * rows + h * half, half), half)]

        if near:
            @pl.when(oc == chip)
            def _():
                pltpu.make_async_copy(src, dst, s_x.at[late, chip]).start()

        @pl.when(wanted)
        def _():
            remote(src, dst, s_xsend.at[m], s_x.at[late, chip], dev(oc, core)).start()

    def finish(m):
        slot = m % 3
        oc = owner_chip(m)
        late = m // chips
        wait_bytes(fin.at[m], s_fin.at[m])
        wait_bytes(momin.at[m % 2], s_mom.at[m % 2])
        size = min(CHUNK, half)
        acc = jnp.zeros((8, 128), F32)
        for h in range(2):
            wait_bytes(fsum.at[m, h], s_fsum.at[m, h], "wait_fsum")

            def part(i, acc):
                at = pl.ds(pl.multiple_of(i * size, size), size)
                mom_at = pl.ds(pl.multiple_of(h * half + i * size, size), size)
                total = own[slot, 2 + h, at].astype(F32) + fin[m, h, 2, at].astype(F32)
                total = total + (fin[m, h, 0, at].astype(F32) + fin[m, h, 1, at].astype(F32))
                total = total + fsum[m, h, at]
                new = MOMENTUM_COEF * momin[m % 2, mom_at] + total
                fsum[m, h, at] = new
                fin[m, h, 0, at] = new.astype(BF16)
                square = new * new
                for r in range(0, size, 8):
                    for q in range(0, cols, 128):
                        acc = acc + square[r:r + 8, q:q + 128]
                return acc

            acc = lax.fori_loop(0, half // size, part, acc)
            if h == 1:
                nsend[m] = acc
                sum_to = ninbox.at[late, me]

                @pl.when(oc == chip)
                def _():
                    pltpu.make_async_copy(nsend.at[m], sum_to, s_n.at[late]).start()
                    remote(nsend.at[m], sum_to, s_nsend.at[m], s_n.at[late], mate).start()

                @pl.when(oc != chip)
                def _():
                    for kk in range(CORES):
                        remote(nsend.at[m], sum_to, s_nsend.at[m], s_n.at[late], dev(oc, kk)).start()

            @pl.when((late == 0) | (m == n_mats - 1))
            def _():
                forward(m, h)

    first, second = pl.ds(0, hr), pl.ds(hr, hr)

    def to_mate(g, buf, at):
        return remote(buf.at[first, at], buf.at[second, at], s_xps.at[g], s_xp.at[g], mate)

    def ns_begin(e):
        g, buf = e * NS_ITERS, (xbuf0, xbuf1)[(e * NS_ITERS) % 2]
        wait_bytes(ninbox.at[e], s_n.at[e], "wait_n")
        total = jnp.sum(ninbox[e], axis=0)
        total = jnp.sum(jnp.sum(total, axis=0, keepdims=True), axis=1, keepdims=True)
        bound = jnp.sqrt(total) + NORM_EPS

        @pl.loop(0, chips)
        def _(step):
            away = jnp.where(step == 2, 3, jnp.where(step == 3, 2, step))
            b = (chip + away) % chips
            here = pl.ds(pl.multiple_of(b * rows, rows), rows)
            wait_bytes(xin.at[e, here], s_x.at[e, b], "wait_x")

            @pl.loop(0, rows // CHUNK)
            def _(i):
                at = pl.ds(pl.multiple_of(b * rows + i * CHUNK, CHUNK), CHUNK)
                buf[at] = (xin[e, at].astype(F32) / bound).astype(BF16)
            there = pl.ds(pl.multiple_of(hr + b * rows, rows), rows)
            remote(buf.at[here], buf.at[there], s_xps.at[g], s_xp.at[g], mate).start()

    def ns_iter(g, par, last, late):
        cur, nxt, col = ((xbuf0, xbuf1, colo0), (xbuf1, xbuf0, colo1))[par]
        transposed = (((1,), (1,)), ((), ()))
        diag = remote(row.at[:, first], col.at[second], s_aps.at[g], s_ap.at[g], mate)

        with jax.named_scope("gram"):
            prod = lax.dot_general(cur[first], cur[first], transposed, preferred_element_type=F32)
            row[:, first] = prod.astype(BF16)
            diag.start()
        wait_bytes(cur.at[second], s_xp.at[g], "wait_xp")
        with jax.named_scope("squares"):
            prod = lax.dot_general(cur[first], cur[second], transposed, preferred_element_type=F32)
            prod = prod.astype(BF16)
            row[:, second] = prod
            col[first] = prod
            prod = lax.dot_general(row[...], row[...], transposed, preferred_element_type=F32)
            poly[:, first] = (COEF_B * row[:, first].astype(F32) + COEF_C * prod).astype(BF16)
        if par == NS_ITERS % 2 and not last:
            @pl.when(g == NS_ITERS)
            def _():
                give_back(0, xin.at[0], pl.ds(0, cols))
        wait_bytes(col.at[second], s_ap.at[g], "wait_ap")
        with jax.named_scope("newx"):
            prod = jnp.dot(row[...], col[...], preferred_element_type=F32)
            poly[:, second] = (COEF_B * row[:, second].astype(F32) + COEF_C * prod).astype(BF16)
            wide = cols // X_PARTS
            for j in range(X_PARTS):
                at = pl.ds(j * wide, wide)
                prod = jnp.dot(poly[...], cur[:, at], preferred_element_type=F32)
                nxt[first, at] = (COEF_A * cur[first, at].astype(F32) + prod).astype(BF16)
                if not last:
                    to_mate(g + 1, nxt, at).start()
                elif late:
                    give_back(1, nxt, at)
        if last and not late:
            keep = pltpu.make_async_copy(nxt.at[first], xin.at[0], s_keep)
            keep.start()
            keep.wait()
        diag.wait_send()
        wait_bytes(cur.at[first], s_xps.at[g])

    def give_back(e, src, at):
        mat = my_mat(e)
        dst = ret.at[mat, :, at]

        def block(c):
            return src.at[pl.ds(pl.multiple_of(c * rows, rows), rows), at]

        for i in range(1, chips):
            c = (chip + i) % chips
            remote(block(c), dst, s_rsend.at[e], s_ret.at[mat], dev(c, core)).start()
        pltpu.make_async_copy(block(chip), dst, s_ret.at[mat]).start()

    def early_done(s):
        return jnp.clip(ITERS_PER_STEP * (s - chip - 2), 0, NS_ITERS)

    barrier = pltpu.get_barrier_semaphore()
    for i in range(1, group):
        pl.semaphore_signal(barrier, inc=1, device_id={"data": (me + i) % group}, device_id_type=MESH)
    pl.semaphore_wait(barrier, group - 1)

    @pl.loop(0, AHEAD)
    def _(m):
        issue_raw(m)
    load_own(0)
    pltpu.make_async_copy(w_ref, wbuf, s_wload).start()

    @pl.loop(0, n_mats + 2)
    def _(s):
        @pl.when(s + AHEAD < n_mats)
        def _():
            issue_raw(s + AHEAD)

        @pl.when(s + 1 < n_mats)
        def _():
            load_own(s + 1)

        @pl.when(s < n_mats)
        def _():
            pltpu.make_async_copy(mom_ref.at[s], momin.at[s % 2], s_mom.at[s % 2]).start()
            merge(s)

        last = s == n_mats + 1
        lo = jnp.where(s >= n_mats, early_done(n_mats - 1), early_done(s - 1))
        hi = jnp.where(last, 2 * NS_ITERS, jnp.where(s >= n_mats, lo, early_done(s)))

        def run(g, carry):
            @pl.when(g == 0)
            def _():
                ns_begin(0)

            @pl.when(g == NS_ITERS)
            def _():
                ns_begin(1)

            end = g % NS_ITERS == NS_ITERS - 1
            for par in range(2):
                @pl.when((g % 2 == par) & jnp.logical_not(end))
                def _():
                    ns_iter(g, par, False, False)
            for e in range(2):
                @pl.when(g == (e + 1) * NS_ITERS - 1)
                def _():
                    ns_iter(g, ((e + 1) * NS_ITERS - 1) % 2, True, e == 1)
            return carry
        lax.fori_loop(lo, hi, run, 0)

        @pl.when((s >= 1) & (s <= n_mats))
        def _():
            finish(s - 1)

        for when, near in ((n_mats - 1, True), (n_mats, False)):
            @pl.when(s == when)
            def _():
                @pl.loop(chips, n_mats - 1)
                def _(m):
                    for h in range(2):
                        forward(m, h, near=near, distant=not near)

    wait_bytes(wbuf, s_wload)

    @pl.loop(0, n_mats)
    def _(m):
        done = g_ref.at[0, m, pl.ds(0, 12 * half)]
        wait_bytes(done, s_gsend.at[m])

        @pl.when(owner_chip(m) == chip)
        def _():
            wait_bytes(nsend.at[0], s_nsend.at[m])

        @pl.when(owner_chip(m) != chip)
        def _():
            wait_bytes(ret.at[m], s_xsend.at[m])
            wait_bytes(nsend.at[pl.ds(0, CORES)], s_nsend.at[m])
    for m in range(n_mats - 2, n_mats):
        for h in range(2):
            merge_copy(m, h).wait_send()

    @pl.loop(0, n_mats)
    def _(m):
        wait_bytes(ret.at[m], s_ret.at[m], "wait_ret")
    for e in range(2):
        wait_bytes(xin.at[e, pl.ds(0, (chips - 1) * rows)], s_rsend.at[e])


def finish_kernel(scale, w_ref, mom_ref, x_ref, w_out, mom_out, wnew, sem):
    n_mats, rows, _ = w_ref.shape
    copies = [pltpu.make_async_copy(mom_ref.at[pl.ds(m, 2)], mom_out.at[pl.ds(m, 2)], sem.at[m]) for m in range(0, n_mats, 2)]
    for copy in copies:
        copy.start()
    for m in range(n_mats):
        @pl.loop(0, rows // CHUNK)
        def _(i):
            at = pl.ds(pl.multiple_of(i * CHUNK, CHUNK), CHUNK)
            w = w_ref[m, at]
            wnew[m, at] = w - LEARN_RATE * (x_ref[m, at].astype(F32) * scale + WEIGHT_DECAY * w)
        copies.append(pltpu.make_async_copy(wnew.at[m], w_out.at[m], sem.at[n_mats + m]))
        copies[-1].start()
    for copy in copies:
        copy.wait()


def solution(mesh):
    group = mesh.shape['data']
    row_spec = P('stage', 'data', None)
    grad_spec = P(('stage', 'data'), None, None, None)

    def local_step(w_rows, mom_rows, grad_full):
        n_mats, rows, cols = w_rows.shape
        half = rows // 2
        n_rows = rows * group
        chips = group // CORES
        hr = n_rows // CORES
        scale = 0.2 * math.sqrt(max(n_rows, cols))
        hbm = pl.BlockSpec(memory_space=pl.ANY)
        vmem = pl.BlockSpec(memory_space=pltpu.VMEM)
        dma = pltpu.SemaphoreType.DMA
        flops = NS_ITERS * (4 * n_rows * n_rows * cols + 2 * n_rows ** 3)
        mom_new, w_held, x_rows = pl.pallas_call(
            functools.partial(fused_kernel, group),
            out_shape=(pltpu.VMEM((n_mats, 2, half, cols), F32), pltpu.VMEM(w_rows.shape, F32), pltpu.VMEM(w_rows.shape, BF16)),
            in_specs=[hbm] * 3,
            out_specs=(vmem, vmem, vmem),
            scratch_shapes=[
                pltpu.VMEM((MG_SLOTS, 2, 3, half, cols), BF16),
                pltpu.VMEM((n_mats, 2, 3, half, cols), BF16),
                pltpu.VMEM((3, 4, half, cols), BF16),
                pltpu.VMEM((2, 2, half, cols), F32),
                pltpu.VMEM((2, rows, cols), F32),
                pltpu.VMEM((2, hr, cols), BF16),
                pltpu.VMEM((n_rows, cols), BF16),
                pltpu.VMEM((n_rows, cols), BF16),
                pltpu.VMEM((hr, n_rows), BF16),
                pltpu.VMEM((n_rows, hr), BF16),
                pltpu.VMEM((n_rows, hr), BF16),
                pltpu.VMEM((hr, n_rows), BF16),
                pltpu.VMEM((n_mats, 8, 128), F32),
                pltpu.VMEM((2, group, 8, 128), F32),
                dma((n_mats, 2)), dma((n_mats,)), dma((n_mats, 2)), dma((3,)), dma((2, 2)), dma((2,)),
                dma((2, chips)), dma((2,)), dma((n_mats,)),
                dma((n_mats,)), dma((n_mats,)), dma((n_mats,)), dma((2,)), dma, pltpu.SemaphoreType.REGULAR((n_mats,)),
                dma((2 * NS_ITERS,)), dma((2 * NS_ITERS,)), dma((2 * NS_ITERS,)), dma((2 * NS_ITERS,)), dma,
            ],
            compiler_params=pltpu.CompilerParams(collective_id=0, has_side_effects=True, vmem_limit_bytes=43 * 2 ** 20),
            cost_estimate=pl.CostEstimate(flops=flops, bytes_accessed=2 ** 26, transcendentals=0),
            name="muon_step",
        )(w_rows, mom_rows, grad_full)
        mom_new = mom_new.reshape(w_rows.shape)
        return pl.pallas_call(
            functools.partial(finish_kernel, scale),
            out_shape=(jax.ShapeDtypeStruct(w_rows.shape, F32), jax.ShapeDtypeStruct(w_rows.shape, F32)),
            in_specs=[vmem] * 3,
            out_specs=(hbm, hbm),
            scratch_shapes=[pltpu.VMEM(w_rows.shape, F32), dma((2 * n_mats,))],
            compiler_params=pltpu.CompilerParams(vmem_limit_bytes=12 * 2 ** 20),
            cost_estimate=pl.CostEstimate(flops=4 * w_rows.size, bytes_accessed=2 * w_rows.size * 4, transcendentals=0),
            name="finish",
        )(w_held, mom_new, x_rows)

    return jax.shard_map(local_step, mesh=mesh, in_specs=(row_spec, row_spec, grad_spec), out_specs=(row_spec, row_spec), check_vma=False)
```
